8 devices in a mesh: cola: 2 (over z, y), colb: 2 (over x), row: 2 (over core).
Axes of the slice: x: 2, y: 2, z: 1, core: 2. Of those that a mesh axis runs over, the one named last changes fastest.
Arguments:
- inter_mask: int32 [32768, 8192], P('row', ('cola', 'colb'))
- user_emb: bfloat16 [32768, 256], P(('row', 'cola', 'colb'))
- item_emb: bfloat16 [8192, 256], P(('cola', 'colb', 'row'))
- triples: int32 [256, 3], replicated
Outputs:
- output 1: bfloat16 [32768, 256], P(('row', 'cola', 'colb'))
- output 2: bfloat16 [8192, 256], P(('cola', 'colb', 'row'))
- output 3: float32 [], replicated
All inputs are finite; a program needn't handle non-finite values.
Results may differ from the reference program's by a relative error of at most 0.00583716.
Values are sent between devices in bfloat16 or wider.
A program may use at most 1 GiB of HBM per device.

```python
import math
import jax
import jax.numpy as jnp
from jax import lax

USERS = 32768
ITEMS = 8192
EMBED = 256
BATCH = 256
LAYERS = 3
GROUPS = 8
SAME_RATE = 120
CROSS_RATE = 5
RATE_SCALE = 1000
CONTRACT_ROWS = (((0,), (0,)), ((), ()))


def setup_inputs(seed: int = 0) -> dict:
    subkeys = jax.random.split(jax.random.key(seed), 8)
    user_group = jax.random.randint(subkeys[0], (USERS,), 0, GROUPS)
    item_group = jax.random.randint(subkeys[1], (ITEMS,), 0, GROUPS)
    draw_vals = jax.random.randint(subkeys[2], (USERS, ITEMS), 0, RATE_SCALE)
    threshold = jnp.where(user_group[:, None] == item_group[None, :], SAME_RATE, CROSS_RATE)
    inter_mask = (draw_vals < threshold).astype(jnp.int32)
    centers = jax.random.normal(subkeys[3], (GROUPS, EMBED), jnp.float32)
    user_noise = jax.random.normal(subkeys[4], (USERS, EMBED), jnp.float32)
    item_noise = jax.random.normal(subkeys[5], (ITEMS, EMBED), jnp.float32)
    user_emb = jnp.take(centers, user_group, axis=0) + 0.7 * user_noise
    item_emb = jnp.take(centers, item_group, axis=0) + 0.7 * item_noise
    triple_users = jax.random.randint(subkeys[6], (BATCH, 1), 0, USERS)
    triple_items = jax.random.randint(subkeys[7], (BATCH, 2), 0, ITEMS)
    triples = jnp.concatenate([triple_users, triple_items], axis=1).astype(jnp.int32)
    return {'inter_mask': inter_mask, 'user_emb': user_emb.astype(jnp.bfloat16), 'item_emb': item_emb.astype(jnp.bfloat16), 'triples': triples}


def reference(inter_mask, user_emb, item_emb, triples):
    deg_user = jnp.maximum(jnp.sum(inter_mask, axis=1), 1).astype(jnp.float32)
    deg_item = jnp.maximum(jnp.sum(inter_mask, axis=0), 1).astype(jnp.float32)
    weights = (lax.rsqrt(deg_user)[:, None] * inter_mask.astype(jnp.float32)) * lax.rsqrt(deg_item)[None, :]
    adjacency = weights.astype(jnp.bfloat16)
    user_cur = user_emb
    item_cur = item_emb
    user_total = user_emb.astype(jnp.float32)
    item_total = item_emb.astype(jnp.float32)
    for layer_idx in range(LAYERS):
        user_next = jnp.dot(adjacency, item_cur, preferred_element_type=jnp.float32).astype(jnp.bfloat16)
        item_next = lax.dot_general(adjacency, user_cur, CONTRACT_ROWS, preferred_element_type=jnp.float32).astype(jnp.bfloat16)
        user_cur = user_next
        item_cur = item_next
        user_total = user_total + user_cur.astype(jnp.float32)
        item_total = item_total + item_cur.astype(jnp.float32)
    user_out = (user_total / (LAYERS + 1)).astype(jnp.bfloat16)
    item_out = (item_total / (LAYERS + 1)).astype(jnp.bfloat16)
    user_rows = jnp.take(user_out, triples[:, 0], axis=0).astype(jnp.float32)
    pos_rows = jnp.take(item_out, triples[:, 1], axis=0).astype(jnp.float32)
    neg_rows = jnp.take(item_out, triples[:, 2], axis=0).astype(jnp.float32)
    margin = (jnp.sum(user_rows * pos_rows, axis=1) - jnp.sum(user_rows * neg_rows, axis=1)) / math.sqrt(EMBED)
    loss = jnp.mean(jax.nn.softplus(-margin))
    return user_out, item_out, loss
```

```python
import math
import jax
import jax.numpy as jnp
from jax import lax
from jax.sharding import PartitionSpec as P

LAYERS = 3
USER_AXES = ('row', 'cola', 'colb')
ITEM_AXES = ('cola', 'colb', 'row')
COL_AXES = ('cola', 'colb')
CONTRACT_ROWS = (((0,), (0,)), ((), ()))
SWAP = [(0, 1), (1, 0)]
F32 = jnp.float32
BF16 = jnp.bfloat16


def swap(value, axis):
    return lax.ppermute(value, axis, SWAP)


def owned_rows(emb_table, row_ids, owner_idx):
    shard_rows = emb_table.shape[0]
    is_owned = (row_ids // shard_rows) == owner_idx
    picked = jnp.take(emb_table, row_ids % shard_rows, axis=0)
    return jnp.where(is_owned[:, None], picked, jnp.zeros_like(picked)), is_owned


def gather_users(half0, half1):
    out = {(0, 0, 0): half0, (0, 0, 1): half1}
    out[0, 1, 0] = swap(half0, 'colb')
    out[1, 0, 1] = swap(half1, 'cola')
    out[1, 0, 0] = swap(half0, 'cola')
    out[0, 1, 1] = swap(half1, 'colb')
    out[1, 1, 0] = swap(out[0, 1, 0], 'cola')
    out[1, 1, 1] = swap(out[1, 0, 1], 'colb')
    return out


def scatter_users(blocks, panel):
    def product(dy, dx, half):
        return jnp.dot(blocks[dy, dx, half], panel, preferred_element_type=F32)
    x_far = swap(product(1, 1, 0), 'colb')
    y_far = swap(product(1, 1, 1), 'cola')
    x_near = swap(product(0, 1, 0), 'colb')
    y_near = swap(product(1, 0, 1), 'cola')
    far0 = product(1, 0, 0) + x_far
    far1 = product(0, 1, 1) + y_far
    y_last = swap(far0, 'cola')
    x_last = swap(far1, 'colb')
    half0 = (product(0, 0, 0) + x_near) + y_last
    half1 = (product(0, 0, 1) + y_near) + x_last
    return half0.astype(BF16), half1.astype(BF16)


def solution(mesh):
    row_count = mesh.shape['row']
    colb_count = mesh.shape['colb']
    col_count = mesh.shape['cola'] * colb_count

    def device_program(mask_blk, user_shard, item_shard, triples):
        row_idx = lax.axis_index('row')
        y_idx, x_idx = lax.axis_index('cola'), lax.axis_index('colb')
        col_idx = y_idx * colb_count + x_idx
        shard = user_shard.shape[0]
        half = shard // 2
        keys = [(dy, dx, h) for h in (0, 1) for dy in (0, 1) for dx in (0, 1)]

        def start_of(key):
            dy, dx, h = key
            return ((y_idx ^ dy) * colb_count + (x_idx ^ dx)) * shard + h * half

        user0 = gather_users(user_shard[:half], user_shard[half:])

        def item_panel(own):
            other = swap(own, 'row')
            first = jnp.where(row_idx == 0, own, other)
            second = jnp.where(row_idx == 0, other, own)
            return jnp.concatenate([first, second], axis=0)

        deg_user = jnp.sum(mask_blk, axis=1)
        deg_item = jnp.sum(mask_blk, axis=0)
        deg_item = deg_item + swap(deg_item, 'row')
        deg_user = lax.psum(deg_user, COL_AXES)
        item_scale = lax.rsqrt(jnp.maximum(deg_item, 1).astype(F32))
        user_scale = lax.rsqrt(jnp.maximum(deg_user, 1).astype(F32))
        blocks = {}
        for key in keys:
            part = lax.dynamic_slice_in_dim(mask_blk, start_of(key), half, 0).astype(F32)
            scale = lax.dynamic_slice_in_dim(user_scale, start_of(key), half, 0)
            blocks[key] = lax.optimization_barrier(((scale[:, None] * part) * item_scale[None, :]).astype(BF16))

        def apply_items(users):
            total = None
            for key in keys:
                term = lax.dot_general(blocks[key], users[key], CONTRACT_ROWS, preferred_element_type=F32)
                total = term if total is None else total + term
            items = total.shape[0] // 2
            mine = lax.dynamic_slice_in_dim(total, row_idx * items, items, 0)
            theirs = lax.dynamic_slice_in_dim(total, (1 - row_idx) * items, items, 0)
            return (mine + swap(theirs, 'row')).astype(BF16)

        item1_own = None
        u1 = scatter_users(blocks, item_panel(item_shard))
        v1 = apply_items(user0)
        u2 = scatter_users(blocks, item_panel(v1))
        v2 = apply_items(gather_users(*u1))
        v3 = apply_items(gather_users(*u2))
        u3 = scatter_users(blocks, item_panel(v2))

        def mean(values):
            total = values[0].astype(F32)
            for value in values[1:]:
                total = total + value.astype(F32)
            return (total / (LAYERS + 1)).astype(BF16)

        item_out = mean([item_shard, v1, v2, v3])
        user_halves = [mean([user_shard[i * half:(i + 1) * half], u1[i], u2[i], u3[i]]) for i in (0, 1)]
        user_out = jnp.concatenate(user_halves, axis=0)
        user_owner = row_idx * col_count + col_idx
        item_owner = col_idx * row_count + row_idx
        pos, _ = owned_rows(item_out, triples[:, 1], item_owner)
        neg, _ = owned_rows(item_out, triples[:, 2], item_owner)
        rows = lax.psum(jnp.stack([pos, neg]).astype(F32), USER_AXES)
        mine, is_mine = owned_rows(user_out, triples[:, 0], user_owner)
        mine = mine.astype(F32)
        margin = (jnp.sum(mine * rows[0], axis=1) - jnp.sum(mine * rows[1], axis=1)) / math.sqrt(mine.shape[1])
        terms = jnp.where(is_mine, jax.nn.softplus(-margin), 0.0)
        loss = lax.psum(jnp.sum(terms), USER_AXES) / triples.shape[0]
        return user_out, item_out, loss

    return jax.shard_map(device_program, mesh=mesh, in_specs=(P('row', COL_AXES), P(USER_AXES, None), P(ITEM_AXES, None), P()), out_specs=(P(USER_AXES, None), P(ITEM_AXES, None), P()), check_vma=False)
```

```python
import functools
import math
import jax
import jax.numpy as jnp
from jax import lax
from jax.experimental import pallas as pl
from jax.experimental.pallas import tpu as pltpu
from jax.sharding import PartitionSpec as P

LAYERS = 3
USER_AXES = ('row', 'cola', 'colb')
ITEM_AXES = ('cola', 'colb', 'row')
COL_AXES = ('cola', 'colb')
F32 = jnp.float32
BF16 = jnp.bfloat16
CONTRACT_ROWS = (((0,), (0,)), ((), ()))
CONTRACT_COLS = (((1,), (1,)), ((), ()))
BUILD = 256
TILE = 512
CHUNK = 32
DEEP = pl.Buffered(4)
OUT = pl.Buffered(2)
LANES = 128


def kernel(dims, mask, user0, item0, triples, user_out, item_out, loss_out, adj, upan, pbuf, precv, sbuf,
           vpan, acc, qrecv, vtot, us, uscol, isc, degu, drecv, degi, degi_recv, sel, selb, selrecv, mine, lsend, lrecv,
           ag_send, ag_recv, rs_send, rs_recv, v_send, v_recv, q_send, q_recv, d_send, d_recv, e_send, e_recv, l_send, l_recv):
    half, items, own_items, dim = dims
    x, y, r = lax.axis_index('colb'), lax.axis_index('cola'), lax.axis_index('row')
    to = {'x': {'colb': 1 - x}, 'y': {'cola': 1 - y}, 'r': {'row': 1 - r},
          'xy': {'colb': 1 - x, 'cola': 1 - y}}
    pending = []
    batch = triples.shape[0]

    def send(src, dst, direction, send_sem, recv_sem):
        copy = pltpu.make_async_remote_copy(src_ref=src, dst_ref=dst, send_sem=send_sem, recv_sem=recv_sem,
                                            device_id=to[direction], device_id_type=pl.DeviceIdType.MESH)
        copy.start()
        pending.append(copy)
        return copy

    def finish(copy):
        copy.wait_send()
        pending[:] = [other for other in pending if other is not copy]

    barrier = pltpu.get_barrier_semaphore()
    for direction in to:
        pl.semaphore_signal(barrier, inc=1, device_id=to[direction], device_id_type=pl.DeviceIdType.MESH)
    pl.semaphore_wait(barrier, 4)

    def own(k, h):
        return user0.at[h] if k == 0 else upan.at[k, 6 + h]

    def gather_start(k):
        return [send(own(k, 0), upan.at[k, 2], 'x', ag_send.at[k, 0], ag_recv.at[k, 0]),
                send(own(k, 1), upan.at[k, 3], 'y', ag_send.at[k, 1], ag_recv.at[k, 1]),
                send(own(k, 0), upan.at[k, 4], 'y', ag_send.at[k, 2], ag_recv.at[k, 2]),
                send(own(k, 1), upan.at[k, 5], 'x', ag_send.at[k, 3], ag_recv.at[k, 3])]

    def gather_forward(k, copies):
        copies[0].wait_recv()
        far0 = send(upan.at[k, 2], upan.at[k, 0], 'y', ag_send.at[k, 4], ag_recv.at[k, 4])
        copies[1].wait_recv()
        far1 = send(upan.at[k, 3], upan.at[k, 1], 'x', ag_send.at[k, 5], ag_recv.at[k, 5])
        return copies[2:] + [far0, far1]

    def wait_all(copies):
        for copy in copies:
            copy.wait_recv()

    gather0 = gather_start(0)
    vpan[0, r] = item0[...]
    item_copy = send(item0, vpan.at[0, r], 'r', v_send.at[0], v_recv.at[0])

    def mask_block(pos, tile):
        h, q = lax.rem(pos, 2), lax.div(pos, 2)
        prim, sec = 1 - lax.div(q, 2), 1 - lax.rem(q, 2)
        dx, dy = prim * (1 - h) + sec * h, sec * (1 - h) + prim * h
        shard = lax.rem(y + dy, 2) * 2 + lax.rem(x + dx, 2)
        return (shard * 2 + h) * (half // BUILD) + tile

    degu[...] = jnp.zeros_like(degu)
    degi[...] = jnp.zeros_like(degi)
    acc[...] = jnp.zeros_like(acc)

    def degree_body(m_ref):
        pos, tile = pl.program_id(0), pl.program_id(1)

        def chunk(i, cols):
            m = m_ref[pl.ds(pl.multiple_of(i * CHUNK, CHUNK), CHUNK), :]
            part = m[:, :LANES]
            for j in range(1, items // LANES):
                part = part + m[:, j * LANES:(j + 1) * LANES]
            uscol[pl.ds(pl.multiple_of(i * CHUNK, CHUNK), CHUNK), :] = part.astype(F32)
            for j in range(CHUNK // 8):
                cols = cols + m[j * 8:(j + 1) * 8, :]
            return cols

        cols = lax.fori_loop(0, BUILD // CHUNK, chunk, jnp.zeros((8, items), jnp.int32))
        degi[...] += cols.astype(F32)
        pick = (lax.broadcasted_iota(jnp.int32, (8, LANES), 0) == tile).astype(BF16)
        degu[pos] += lax.dot_general(pick, uscol[...].astype(BF16), CONTRACT_COLS, preferred_element_type=F32)

    pltpu.emit_pipeline(degree_body, grid=(8, half // BUILD),
                        in_specs=[pl.BlockSpec((BUILD, items), lambda p, t: (mask_block(p, t), 0), pipeline_mode=DEEP)])(mask)
    item_deg = send(degi, degi_recv, 'r', d_send.at[0], d_recv.at[0])
    user_deg = send(degu, drecv.at[0], 'x', d_send.at[1], d_recv.at[1])
    user_deg.wait_recv()
    finish(user_deg)
    for pos in range(8):
        us[pos] = degu[pos] + drecv[0, pos ^ (2 if pos % 2 else 4)]
    user_deg2 = send(us, drecv.at[1], 'y', d_send.at[2], d_recv.at[2])
    rest0 = gather_forward(0, gather0)
    item_deg.wait_recv()
    total = jnp.sum(degi[...] + degi_recv[...], axis=0, keepdims=True)
    isc[...] = lax.rsqrt(jnp.maximum(total, 1.0))
    user_deg2.wait_recv()
    finish(user_deg2)
    for pos in range(8):
        degu[pos] = lax.rsqrt(jnp.maximum(us[pos] + drecv[1, pos ^ (4 if pos % 2 else 2)], 1.0))
    item_copy.wait_recv()

    def panel(k):
        return vpan[k].reshape(items, dim)

    def add_items(a_ref, u_ref):
        for j in range(2):
            acc[j] += lax.dot_general(u_ref[...], a_ref[:, j * own_items:(j + 1) * own_items], CONTRACT_ROWS,
                                      preferred_element_type=F32)

    def build(first, count, users):
        def body(m_ref, *refs):
            (u_ref, a_ref, p_ref) = refs if users is not None else (None,) + refs
            pos, tile = pl.program_id(0) + first, pl.program_id(1)
            row = degu[pos, pl.ds(tile, 1), :]
            uscol[...] = jnp.transpose(jnp.broadcast_to(row, (LANES, BUILD)))

            def chunk(i, carry):
                rows = pl.ds(pl.multiple_of(i * CHUNK, CHUNK), CHUNK)
                scale = uscol[rows, :]
                for j in range(items // LANES):
                    cols = slice(j * LANES, (j + 1) * LANES)
                    weight = (scale * m_ref[rows, cols].astype(F32)) * isc[:, cols]
                    a_ref[rows, cols] = weight.astype(BF16)
                return carry

            lax.fori_loop(0, BUILD // CHUNK, chunk, 0)
            p_ref[...] = jnp.dot(a_ref[...], panel(0), preferred_element_type=F32)
            if users is not None:
                add_items(a_ref, u_ref)

        operands = [mask]
        in_specs = [pl.BlockSpec((BUILD, items), lambda p, t: (mask_block(p + first, t), 0), pipeline_mode=DEEP)]
        if users is not None:
            ref, start = users
            operands.append(ref)
            in_specs.append(pl.BlockSpec((None, BUILD, dim), lambda p, t: (p + (first - start), t, 0), pipeline_mode=DEEP))
        pltpu.emit_pipeline(body, grid=(count, half // BUILD), in_specs=in_specs,
                            out_specs=[pl.BlockSpec((None, BUILD, items), lambda p, t: (p + first, t, 0), pipeline_mode=OUT),
                                       pl.BlockSpec((None, BUILD, dim), lambda p, t: (p + first, t, 0), pipeline_mode=OUT)])(*operands, adj, pbuf.at[0])

    def multiply(k, first, count):
        def body(a_ref, p_ref):
            p_ref[...] = jnp.dot(a_ref[...], panel(k), preferred_element_type=F32)
        pltpu.emit_pipeline(body, grid=(count, half // TILE),
                            in_specs=[pl.BlockSpec((None, TILE, items), lambda p, t: (p + first, t, 0), pipeline_mode=DEEP)],
                            out_specs=[pl.BlockSpec((None, TILE, dim), lambda p, t: (p + first, t, 0), pipeline_mode=OUT)])(adj, pbuf.at[k])

    def accumulate(k, count):
        pltpu.emit_pipeline(add_items, grid=(count, half // TILE),
                            in_specs=[pl.BlockSpec((None, TILE, items), lambda p, t: (p, t, 0), pipeline_mode=DEEP),
                                      pl.BlockSpec((None, TILE, dim), lambda p, t: (p, t, 0), pipeline_mode=DEEP)])(adj, upan.at[k])

    def scatter_send(k, pos):
        return send(pbuf.at[k, pos], precv.at[k, pos], 'y' if pos % 2 else 'x', rs_send.at[k, pos], rs_recv.at[k, pos])

    tile_spec = pl.BlockSpec((TILE, dim), lambda t: (t, 0), pipeline_mode=DEEP)
    out_spec = pl.BlockSpec((TILE, dim), lambda t: (t, 0), pipeline_mode=OUT)

    def scatter_last(k, h, far):
        far.wait_recv()

        def body(p_ref, r_ref, s_ref):
            s_ref[...] = p_ref[...] + r_ref[...]
        pltpu.emit_pipeline(body, grid=(half // TILE,), in_specs=[tile_spec] * 2, out_specs=[out_spec])(
            pbuf.at[k, 4 + h], precv.at[k, h], sbuf.at[k, h])
        return send(sbuf.at[k, h], precv.at[k, 4 + h], 'x' if h else 'y', rs_send.at[k, 4 + h], rs_recv.at[k, 4 + h])

    def scatter_finish(k, h, near, last):
        near.wait_recv()
        last.wait_recv()

        def body(p_ref, n_ref, l_ref, u_ref):
            u_ref[...] = ((p_ref[...] + n_ref[...]) + l_ref[...]).astype(BF16)
        pltpu.emit_pipeline(body, grid=(half // TILE,), in_specs=[tile_spec] * 3, out_specs=[out_spec])(
            pbuf.at[k, 6 + h], precv.at[k, 2 + h], precv.at[k, 4 + h], upan.at[k + 1, 6 + h])

    def item_layer(k):
        copy = send(acc.at[1 - r], qrecv.at[k - 1], 'r', q_send.at[k - 1], q_recv.at[k - 1])
        copy.wait_recv()
        rows = jnp.transpose(acc[r] + qrecv[k - 1]).astype(BF16)
        vtot[...] += rows.astype(F32)
        finish(copy)
        if k < LAYERS:
            vpan[k, r] = rows
            other = send(vpan.at[k, r], vpan.at[k, r], 'r', v_send.at[k], v_recv.at[k])
            acc[...] = jnp.zeros_like(acc)
            other.wait_recv()

    vtot[...] = item0[...].astype(F32)
    far, near = {}, {}
    build(0, 1, None)
    far[0, 0] = scatter_send(0, 0)
    build(1, 1, None)
    far[0, 1] = scatter_send(0, 1)
    build(2, 1, (upan.at[0], 0))
    near[0, 0] = scatter_send(0, 2)
    build(3, 1, (upan.at[0], 0))
    near[0, 1] = scatter_send(0, 3)
    wait_all(rest0[:2])
    build(4, 2, (upan.at[0], 0))
    build(6, 2, (user0, 6))
    wait_all(rest0[2:])
    last0 = [scatter_last(0, h, far[0, h]) for h in (0, 1)]
    accumulate(0, 2)
    item_layer(1)
    for pos in range(2):
        multiply(1, pos, 1)
        far[1, pos] = scatter_send(1, pos)
    multiply(1, 2, 6)
    for h in (0, 1):
        scatter_finish(0, h, near[0, h], last0[h])
    gather1 = gather_start(1)
    rest1 = gather_forward(1, gather1)
    for pos in (2, 3):
        near[1, pos % 2] = scatter_send(1, pos)
    last1 = [scatter_last(1, h, far[1, h]) for h in (0, 1)]
    wait_all(rest1)
    accumulate(1, 8)
    item_layer(2)
    for pos in range(2):
        multiply(2, pos, 1)
        far[2, pos] = scatter_send(2, pos)
    multiply(2, 2, 6)
    for h in (0, 1):
        scatter_finish(1, h, near[1, h], last1[h])
    gather2 = gather_start(2)
    rest2 = gather_forward(2, gather2)
    last2 = [scatter_last(2, h, far[2, h]) for h in (0, 1)]
    wait_all(rest2)
    accumulate(2, 8)
    item_layer(3)

    out_rows = (vtot[...] / (LAYERS + 1)).astype(BF16)
    item_out[...] = out_rows
    item_base = ((y * 2 + x) * 2 + r) * own_items
    for j in range(2):
        hit = (triples[:, 1 + j:2 + j] - item_base) == lax.broadcasted_iota(jnp.int32, (batch, own_items), 1)
        selb[j] = jnp.dot(hit.astype(BF16), out_rows, preferred_element_type=F32).astype(BF16)
    core = send(selb.at[1 - r], selrecv.at[0], 'r', e_send.at[0], e_recv.at[0])
    core.wait_recv()
    sel[...] = selb[r] + selrecv[0]
    shared = [send(sel, selrecv.at[i], direction, e_send.at[i], e_recv.at[i]) for i, direction in ((1, 'x'), (2, 'y'), (3, 'xy'))]
    for pos in (2, 3):
        near[2, pos % 2] = scatter_send(2, pos)
    wait_all(shared)
    finish(core)
    selb[r] = (sel[...] + selrecv[1]) + (selrecv[2] + selrecv[3])
    back = send(selb.at[r], selrecv.at[4], 'r', e_send.at[4], e_recv.at[4])
    back.wait_recv()

    user_base = ((r * 2 + y) * 2 + x) * (2 * half)
    mine[...] = jnp.zeros_like(mine)
    for h in (0, 1):
        near[2, h].wait_recv()
        last2[h].wait_recv()

        def body(p_ref, n_ref, l_ref, u0_ref, u1_ref, u2_ref, o_ref, h=h):
            last_user = ((p_ref[...] + n_ref[...]) + l_ref[...]).astype(BF16)
            rows = u0_ref[...].astype(F32) + u1_ref[...].astype(F32)
            rows = (rows + u2_ref[...].astype(F32)) + last_user.astype(F32)
            rows = (rows / (LAYERS + 1)).astype(BF16)
            o_ref[...] = rows
            first = user_base + h * half + pl.program_id(0) * TILE
            hit = (triples[:, 0:1] - first) == lax.broadcasted_iota(jnp.int32, (batch, TILE), 1)
            mine[...] += jnp.dot(hit.astype(BF16), rows, preferred_element_type=F32)
        pltpu.emit_pipeline(body, grid=(half // TILE,), in_specs=[tile_spec] * 6, out_specs=[out_spec])(
            pbuf.at[2, 6 + h], precv.at[2, 2 + h], precv.at[2, 4 + h], user0.at[h], upan.at[1, 6 + h], upan.at[2, 6 + h],
            user_out.at[h])
    own_rows, other_rows = selb[r].astype(F32), selrecv[4].astype(F32)
    pos_rows = jnp.where(r == 0, own_rows, other_rows)
    neg_rows = jnp.where(r == 0, other_rows, own_rows)
    rows = mine[...]
    margin = (jnp.sum(rows * pos_rows, axis=1, keepdims=True) - jnp.sum(rows * neg_rows, axis=1, keepdims=True)) / math.sqrt(dim)
    local = triples[:, 0:1] - user_base
    soft = jnp.maximum(-margin, 0.0) + jnp.log1p(jnp.exp(-jnp.abs(margin)))
    terms = jnp.where((local >= 0) & (local < 2 * half), soft, 0.0)
    value = jnp.broadcast_to(jnp.sum(terms, axis=0, keepdims=True), (8, LANES))
    for i, direction in enumerate('rxy'):
        lsend[i] = value
        send(lsend.at[i], lrecv.at[i], direction, l_send.at[i], l_recv.at[i]).wait_recv()
        value = value + lrecv[i]
    loss_out[...] = value[0:1, 0:1] / batch
    for copy in pending:
        copy.wait_send()


def solution(mesh):
    def device_program(mask_blk, user_shard, item_shard, triples):
        shard, dim = user_shard.shape
        half, items, own_items, batch = shard // 2, mask_blk.shape[1], item_shard.shape[0], triples.shape[0]
        hbm = pl.BlockSpec(memory_space=pl.ANY)
        vmem = pl.BlockSpec(memory_space=pltpu.VMEM)
        shapes = [((2, half, dim), BF16), ((own_items, dim), BF16), ((1, 1), F32), ((8, half, items), BF16),
                  ((LAYERS, 8, half, dim), BF16), ((LAYERS, 8, half, dim), F32), ((LAYERS, 6, half, dim), F32),
                  ((LAYERS, 2, half, dim), F32)]
        dma = pltpu.SemaphoreType.DMA
        outs = pl.pallas_call(
            functools.partial(kernel, (half, items, own_items, dim)),
            out_shape=[jax.ShapeDtypeStruct(*shape) for shape in shapes],
            in_specs=[hbm, hbm, vmem, vmem],
            out_specs=[hbm, vmem, vmem] + [hbm] * 5,
            scratch_shapes=[
                pltpu.VMEM((LAYERS, 2, own_items, dim), BF16), pltpu.VMEM((2, dim, own_items), F32),
                pltpu.VMEM((LAYERS, dim, own_items), F32), pltpu.VMEM((own_items, dim), F32),
                pltpu.VMEM((8, 8, BUILD), F32), pltpu.VMEM((BUILD, LANES), F32), pltpu.VMEM((1, items), F32),
                pltpu.VMEM((8, 8, BUILD), F32), pltpu.VMEM((2, 8, 8, BUILD), F32),
                pltpu.VMEM((8, items), F32), pltpu.VMEM((8, items), F32),
                pltpu.VMEM((batch, dim), BF16), pltpu.VMEM((2, batch, dim), BF16), pltpu.VMEM((5, batch, dim), BF16),
                pltpu.VMEM((batch, dim), F32), pltpu.VMEM((3, 8, LANES), F32), pltpu.VMEM((3, 8, LANES), F32),
                dma((LAYERS, 6)), dma((LAYERS, 6)), dma((LAYERS, 6)), dma((LAYERS, 6)), dma((LAYERS,)), dma((LAYERS,)),
                dma((LAYERS,)), dma((LAYERS,)), dma((3,)), dma((3,)), dma((5,)), dma((5,)), dma((3,)), dma((3,))],
            compiler_params=pltpu.CompilerParams(collective_id=0, has_side_effects=True, vmem_limit_bytes=60 * 1024 * 1024),
        )(mask_blk, user_shard.reshape(2, half, dim), item_shard, triples)
        return outs[0].reshape(shard, dim), outs[1], outs[2].reshape(())

    return jax.shard_map(device_program, mesh=mesh, in_specs=(P('row', COL_AXES), P(USER_AXES, None), P(ITEM_AXES, None), P()), out_specs=(P(USER_AXES, None), P(ITEM_AXES, None), P()), check_vma=False)
```

```python
import functools
import itertools
import math
import jax
import jax.numpy as jnp
from jax import lax
from jax.experimental import pallas as pl
from jax.experimental.pallas import tpu as pltpu
from jax.sharding import PartitionSpec as P

LAYERS = 3
USER_AXES = ('row', 'cola', 'colb')
ITEM_AXES = ('cola', 'colb', 'row')
COL_AXES = ('cola', 'colb')
F32 = jnp.float32
BF16 = jnp.bfloat16
CONTRACT_ROWS = (((0,), (0,)), ((), ()))
CONTRACT_COLS = (((1,), (1,)), ((), ()))
BUILD = 256
TILE = 512
CHUNK = 32
PARTS = 4
DEEP = pl.Buffered(4)
OUT = pl.Buffered(2)
LANES = 128


def kernel(dims, mask, user0, item0, triples, user_out, item_out, loss_out, adj, upan, pbuf, precv, sbuf,
           vpan, acc, qrecv, vtot, us, uscol, isc, degu, drecv, degi, degi_recv, sel, selb, selrecv, mine, lsend, lrecv,
           ids, idcol, base, usum, nearv, outv, iout, local_sem, out_sem,
           ag_send, ag_recv, rs_send, rs_recv, v_send, v_recv, q_send, q_recv, d_send, d_recv, e_send, e_recv, l_send, l_recv):
    half, items, own_items, dim = dims
    x, y, r = lax.axis_index('colb'), lax.axis_index('cola'), lax.axis_index('row')
    to = {'x': {'colb': 1 - x}, 'y': {'cola': 1 - y}, 'r': {'row': 1 - r}}
    others = [{'cola': 1 - y if dy else y, 'colb': 1 - x if dx else x, 'row': 1 - r if dr else r}
              for dy, dx, dr in itertools.product((0, 1), repeat=3) if dy or dx or dr]
    pending = []
    batch = ids.shape[1]

    def send_to(src, dst, device, send_sem, recv_sem):
        copy = pltpu.make_async_remote_copy(src_ref=src, dst_ref=dst, send_sem=send_sem, recv_sem=recv_sem,
                                            device_id=device, device_id_type=pl.DeviceIdType.MESH)
        copy.start()
        pending.append(copy)
        return copy

    def send(src, dst, direction, send_sem, recv_sem):
        return send_to(src, dst, to[direction], send_sem, recv_sem)

    def finish(copy):
        copy.wait_send()
        pending[:] = [other for other in pending if other is not copy]

    item_in = pltpu.make_async_copy(item0, vpan.at[0, r], local_sem.at[0])
    ids_in = pltpu.make_async_copy(triples, ids, local_sem.at[1])
    item_in.start()
    ids_in.start()
    barrier = pltpu.get_barrier_semaphore()
    for device in others:
        pl.semaphore_signal(barrier, inc=1, device_id=device, device_id_type=pl.DeviceIdType.MESH)
    pl.semaphore_wait(barrier, len(others))

    def own(k, h):
        return user0.at[h] if k == 0 else upan.at[k, 6 + h]

    def gather_start(k):
        return [send(own(k, 0), upan.at[k, 2], 'x', ag_send.at[k, 0], ag_recv.at[k, 0]),
                send(own(k, 1), upan.at[k, 3], 'y', ag_send.at[k, 1], ag_recv.at[k, 1]),
                send(own(k, 0), upan.at[k, 4], 'y', ag_send.at[k, 2], ag_recv.at[k, 2]),
                send(own(k, 1), upan.at[k, 5], 'x', ag_send.at[k, 3], ag_recv.at[k, 3])]

    def gather_forward(k, copies):
        copies[0].wait_recv()
        far0 = send(upan.at[k, 2], upan.at[k, 0], 'y', ag_send.at[k, 4], ag_recv.at[k, 4])
        copies[1].wait_recv()
        far1 = send(upan.at[k, 3], upan.at[k, 1], 'x', ag_send.at[k, 5], ag_recv.at[k, 5])
        return copies[2:] + [far0, far1]

    def wait_all(copies):
        for copy in copies:
            copy.wait_recv()

    gather0 = gather_start(0)
    item_in.wait()
    ids_in.wait()
    item_copy = send(item0, vpan.at[0, r], 'r', v_send.at[0], v_recv.at[0])

    def mask_block(pos, tile):
        h, q = lax.rem(pos, 2), lax.div(pos, 2)
        prim, sec = 1 - lax.div(q, 2), 1 - lax.rem(q, 2)
        dx, dy = prim * (1 - h) + sec * h, sec * (1 - h) + prim * h
        shard = lax.rem(y + dy, 2) * 2 + lax.rem(x + dx, 2)
        return (shard * 2 + h) * (half // BUILD) + tile

    degu[...] = jnp.zeros_like(degu)
    degi[...] = jnp.zeros_like(degi)
    acc[...] = jnp.zeros_like(acc)

    def degree_body(m_ref):
        pos, tile = pl.program_id(0), pl.program_id(1)

        def chunk(i, cols):
            m = m_ref[pl.ds(pl.multiple_of(i * CHUNK, CHUNK), CHUNK), :]
            part = m[:, :LANES]
            for j in range(1, items // LANES):
                part = part + m[:, j * LANES:(j + 1) * LANES]
            uscol[pl.ds(pl.multiple_of(i * CHUNK, CHUNK), CHUNK), :] = part.astype(F32)
            for j in range(CHUNK // 8):
                cols = cols + m[j * 8:(j + 1) * 8, :]
            return cols

        cols = lax.fori_loop(0, BUILD // CHUNK, chunk, jnp.zeros((8, items), jnp.int32))
        degi[...] += cols.astype(F32)
        pick = (lax.broadcasted_iota(jnp.int32, (8, LANES), 0) == tile).astype(BF16)
        degu[pos] += lax.dot_general(pick, uscol[...].astype(BF16), CONTRACT_COLS, preferred_element_type=F32)

    pltpu.emit_pipeline(degree_body, grid=(8, half // BUILD),
                        in_specs=[pl.BlockSpec((BUILD, items), lambda p, t: (mask_block(p, t), 0), pipeline_mode=DEEP)])(mask)
    item_deg = send(degi, degi_recv, 'r', d_send.at[0], d_recv.at[0])
    user_deg = send(degu, drecv.at[0], 'x', d_send.at[1], d_recv.at[1])
    user_deg.wait_recv()
    finish(user_deg)
    for pos in range(8):
        us[pos] = degu[pos] + drecv[0, pos ^ (2 if pos % 2 else 4)]
    user_deg2 = send(us, drecv.at[1], 'y', d_send.at[2], d_recv.at[2])
    rest0 = gather_forward(0, gather0)
    item_deg.wait_recv()
    total = jnp.sum(degi[...] + degi_recv[...], axis=0, keepdims=True)
    isc[...] = lax.rsqrt(jnp.maximum(total, 1.0))
    user_deg2.wait_recv()
    finish(user_deg2)
    for pos in range(8):
        degu[pos] = lax.rsqrt(jnp.maximum(us[pos] + drecv[1, pos ^ (4 if pos % 2 else 2)], 1.0))
    item_copy.wait_recv()

    def panel(k):
        return vpan[k].reshape(items, dim)

    def add_items(a_ref, u_ref):
        for j in range(2):
            acc[j] += lax.dot_general(u_ref[...], a_ref[:, j * own_items:(j + 1) * own_items], CONTRACT_ROWS,
                                      preferred_element_type=F32)

    def build(first, count, users, start_tile=0, tiles=half // BUILD):
        def body(m_ref, *refs):
            (u_ref, a_ref, p_ref) = refs if users is not None else (None,) + refs
            pos, tile = pl.program_id(0) + first, pl.program_id(1) + start_tile
            row = degu[pos, pl.ds(tile, 1), :]
            uscol[...] = jnp.transpose(jnp.broadcast_to(row, (LANES, BUILD)))

            def chunk(i, carry):
                rows = pl.ds(pl.multiple_of(i * CHUNK, CHUNK), CHUNK)
                scale = uscol[rows, :]
                for j in range(items // LANES):
                    cols = slice(j * LANES, (j + 1) * LANES)
                    weight = (scale * m_ref[rows, cols].astype(F32)) * isc[:, cols]
                    a_ref[rows, cols] = weight.astype(BF16)
                return carry

            lax.fori_loop(0, BUILD // CHUNK, chunk, 0)
            p_ref[...] = jnp.dot(a_ref[...], panel(0), preferred_element_type=F32)
            if users is not None:
                add_items(a_ref, u_ref)

        operands = [mask]
        in_specs = [pl.BlockSpec((BUILD, items), lambda p, t: (mask_block(p + first, t + start_tile), 0), pipeline_mode=DEEP)]
        if users is not None:
            ref, start = users
            operands.append(ref)
            in_specs.append(pl.BlockSpec((None, BUILD, dim), lambda p, t: (p + (first - start), t + start_tile, 0), pipeline_mode=DEEP))
        pltpu.emit_pipeline(body, grid=(count, tiles), in_specs=in_specs,
                            out_specs=[pl.BlockSpec((None, BUILD, items), lambda p, t: (p + first, t + start_tile, 0), pipeline_mode=OUT),
                                       pl.BlockSpec((None, BUILD, dim), lambda p, t: (p + first, t + start_tile, 0), pipeline_mode=OUT)])(*operands, adj, pbuf.at[0])

    def multiply(k, first, count):
        def body(a_ref, p_ref):
            p_ref[...] = jnp.dot(a_ref[...], panel(k), preferred_element_type=F32)
        pltpu.emit_pipeline(body, grid=(count, half // TILE),
                            in_specs=[pl.BlockSpec((None, TILE, items), lambda p, t: (p + first, t, 0), pipeline_mode=DEEP)],
                            out_specs=[pl.BlockSpec((None, TILE, dim), lambda p, t: (p + first, t, 0), pipeline_mode=OUT)])(adj, pbuf.at[k])

    def accumulate(k, count):
        pltpu.emit_pipeline(add_items, grid=(count, half // TILE),
                            in_specs=[pl.BlockSpec((None, TILE, items), lambda p, t: (p, t, 0), pipeline_mode=DEEP),
                                      pl.BlockSpec((None, TILE, dim), lambda p, t: (p, t, 0), pipeline_mode=DEEP)])(adj, upan.at[k])

    def scatter_send(k, pos, part=0, parts=1):
        rows = pl.ds(part * (half // parts), half // parts)
        dst = nearv.at[pos - 2, rows] if k == LAYERS - 1 and pos >= 2 else precv.at[k, pos, rows]
        return send(pbuf.at[k, pos, rows], dst, 'y' if pos % 2 else 'x', rs_send.at[k, pos, part], rs_recv.at[k, pos, part])

    tile_spec = pl.BlockSpec((TILE, dim), lambda t: (t, 0), pipeline_mode=DEEP)
    out_spec = pl.BlockSpec((TILE, dim), lambda t: (t, 0), pipeline_mode=OUT)

    def scatter_last(k, h, far):
        wait_all(far)

        def body(p_ref, r_ref, s_ref):
            s_ref[...] = p_ref[...] + r_ref[...]
        pltpu.emit_pipeline(body, grid=(half // TILE,), in_specs=[tile_spec] * 2, out_specs=[out_spec])(
            pbuf.at[k, 4 + h], precv.at[k, h], sbuf.at[k, h])
        return send(sbuf.at[k, h], precv.at[k, 4 + h], 'x' if h else 'y', rs_send.at[k, 4 + h, 0], rs_recv.at[k, 4 + h, 0])

    def scatter_finish(k, h, near, last):
        near.wait_recv()
        last.wait_recv()

        def body(p_ref, n_ref, l_ref, u_ref):
            u_ref[...] = ((p_ref[...] + n_ref[...]) + l_ref[...]).astype(BF16)
        pltpu.emit_pipeline(body, grid=(half // TILE,), in_specs=[tile_spec] * 3, out_specs=[out_spec])(
            pbuf.at[k, 6 + h], precv.at[k, 2 + h], precv.at[k, 4 + h], upan.at[k + 1, 6 + h])

    def item_layer(k):
        copy = send(acc.at[1 - r], qrecv.at[k - 1], 'r', q_send.at[k - 1], q_recv.at[k - 1])
        copy.wait_recv()
        rows = jnp.transpose(acc[r] + qrecv[k - 1]).astype(BF16)
        vtot[...] += rows.astype(F32)
        finish(copy)
        if k < LAYERS:
            vpan[k, r] = rows
            other = send(vpan.at[k, r], vpan.at[k, r], 'r', v_send.at[k], v_recv.at[k])
            acc[...] = jnp.zeros_like(acc)
            other.wait_recv()

    vtot[...] = vpan[0, r].astype(F32)
    for j in range(3):
        row = jnp.broadcast_to(ids[j:j + 1, :].astype(F32), (LANES, batch))
        idcol[j] = jnp.transpose(row).astype(jnp.int32)
    far, near = {}, {}
    build(0, 1, None)
    far[0, 0] = [scatter_send(0, 0)]
    far[0, 1] = []
    for part in range(2):
        build(1, 1, None, part * (half // BUILD // 2), half // BUILD // 2)
        far[0, 1].append(scatter_send(0, 1, part, 2))
    build(2, 1, (upan.at[0], 0))
    near[0, 0] = scatter_send(0, 2)
    build(3, 1, (upan.at[0], 0))
    near[0, 1] = scatter_send(0, 3)
    wait_all(rest0[:2])
    build(4, 2, (upan.at[0], 0))
    build(6, 2, (user0, 6))
    wait_all(rest0[2:])
    last0 = [scatter_last(0, h, far[0, h]) for h in (0, 1)]
    accumulate(0, 2)
    item_layer(1)
    for pos in range(2):
        multiply(1, pos, 1)
        far[1, pos] = [scatter_send(1, pos)]
    multiply(1, 2, 6)
    for h in (0, 1):
        scatter_finish(0, h, near[0, h], last0[h])
    gather1 = gather_start(1)
    rest1 = gather_forward(1, gather1)
    for pos in (2, 3):
        near[1, pos % 2] = scatter_send(1, pos)
    last1 = [scatter_last(1, h, far[1, h]) for h in (0, 1)]
    wait_all(rest1)
    accumulate(1, 8)
    item_layer(2)
    for pos in range(2):
        multiply(2, pos, 1)
        far[2, pos] = [scatter_send(2, pos)]
    multiply(2, 2, 6)
    for h in (0, 1):
        scatter_finish(1, h, near[1, h], last1[h])
    gather2 = gather_start(2)
    rest2 = gather_forward(2, gather2)
    last2 = [scatter_last(2, h, far[2, h]) for h in (0, 1)]
    wait_all(rest2)
    accumulate(2, 8)
    item_layer(3)

    out_rows = (vtot[...] / (LAYERS + 1)).astype(BF16)
    iout[...] = out_rows
    item_done = pltpu.make_async_copy(iout, item_out, local_sem.at[2])
    item_done.start()
    item_base = ((y * 2 + x) * 2 + r) * own_items
    for j in range(2):
        hit = (idcol[1 + j, :, 0:1] - item_base) == lax.broadcasted_iota(jnp.int32, (batch, own_items), 1)
        selb[j] = jnp.dot(hit.astype(BF16), out_rows, preferred_element_type=F32).astype(BF16)
    core = send(selb.at[1 - r], selrecv.at[0], 'r', e_send.at[0], e_recv.at[0])
    core.wait_recv()
    sel[0] = selb[r] + selrecv[0]
    xrow = send(sel.at[0], selrecv.at[1], 'x', e_send.at[1], e_recv.at[1])
    parts = {2: [scatter_send(2, 2, 0, PARTS)], 3: [scatter_send(2, 3, 0, PARTS)]}
    xrow.wait_recv()
    sel[1] = sel[0] + selrecv[1]
    yrow = send(sel.at[1], selrecv.at[2], 'y', e_send.at[2], e_recv.at[2])
    for part in range(1, PARTS):
        for pos in (2, 3):
            parts[pos].append(scatter_send(2, pos, part, PARTS))

    for h in (0, 1):
        last2[h].wait_recv()

        def body(p_ref, l_ref, u0_ref, u1_ref, u2_ref, h=h):
            rows = pl.ds(pl.multiple_of(pl.program_id(0) * TILE, TILE), TILE)
            base[h, rows, :] = p_ref[...] + l_ref[...]
            usum[h, rows, :] = (u0_ref[...].astype(F32) + u1_ref[...].astype(F32)) + u2_ref[...].astype(F32)
        pltpu.emit_pipeline(body, grid=(half // TILE,), in_specs=[tile_spec] * 5)(
            pbuf.at[2, 6 + h], precv.at[2, 4 + h], user0.at[h], upan.at[1, 6 + h], upan.at[2, 6 + h])
    yrow.wait_recv()
    finish(core)
    selb[r] = sel[1] + selrecv[2]
    back = send(selb.at[r], selrecv.at[3], 'r', e_send.at[3], e_recv.at[3])
    back.wait_recv()

    user_base = ((r * 2 + y) * 2 + x) * (2 * half)
    local = idcol[0, :, 0:1] - user_base
    mine[...] = jnp.zeros_like(mine)
    size = half // PARTS
    stores = []
    for part in range(PARTS):
        rows = pl.ds(part * size, size)
        for h in (0, 1):
            parts[2 + h][part].wait_recv()
            last_user = (base[h, rows, :] + nearv[h, rows, :]).astype(BF16)
            mean = ((usum[h, rows, :] + last_user.astype(F32)) / (LAYERS + 1)).astype(BF16)
            outv[h, rows, :] = mean
            store = pltpu.make_async_copy(outv.at[h, rows], user_out.at[h, rows], out_sem.at[h, part])
            store.start()
            stores.append(store)
            hit = (local - (h * half + part * size)) == lax.broadcasted_iota(jnp.int32, (batch, size), 1)
            mine[...] += jnp.dot(hit.astype(BF16), mean, preferred_element_type=F32)
    own_rows, other_rows = selb[r].astype(F32), selrecv[3].astype(F32)
    pos_rows = jnp.where(r == 0, own_rows, other_rows)
    neg_rows = jnp.where(r == 0, other_rows, own_rows)
    rows = mine[...]
    margin = (jnp.sum(rows * pos_rows, axis=1, keepdims=True) - jnp.sum(rows * neg_rows, axis=1, keepdims=True)) / math.sqrt(dim)
    soft = jnp.maximum(-margin, 0.0) + jnp.log1p(jnp.exp(-jnp.abs(margin)))
    terms = jnp.where((local >= 0) & (local < 2 * half), soft, 0.0)
    lsend[...] = jnp.broadcast_to(jnp.sum(terms, axis=0, keepdims=True), (8, LANES))
    shared = [send_to(lsend, lrecv.at[i], device, l_send.at[i], l_recv.at[i]) for i, device in enumerate(others)]
    for store in stores:
        store.wait()
    item_done.wait()
    for copy in pending:
        copy.wait_send()
    wait_all(shared)
    level = [lsend[...]] + [lrecv[i] for i in range(len(others))]
    while len(level) > 1:
        level = [level[i] + level[i + 1] for i in range(0, len(level), 2)]
    loss_out[...] = level[0][0:1, 0:1] / batch


def solution(mesh):
    def device_program(mask_blk, user_shard, item_shard, triples):
        shard, dim = user_shard.shape
        half, items, own_items, batch = shard // 2, mask_blk.shape[1], item_shard.shape[0], triples.shape[0]
        hbm = pl.BlockSpec(memory_space=pl.ANY)
        vmem = pl.BlockSpec(memory_space=pltpu.VMEM)
        shapes = [((2, half, dim), BF16), ((own_items, dim), BF16), ((1, 1), F32), ((8, half, items), BF16),
                  ((LAYERS, 8, half, dim), BF16), ((LAYERS, 8, half, dim), F32), ((LAYERS, 6, half, dim), F32),
                  ((LAYERS, 2, half, dim), F32)]
        dma = pltpu.SemaphoreType.DMA
        outs = pl.pallas_call(
            functools.partial(kernel, (half, items, own_items, dim)),
            out_shape=[jax.ShapeDtypeStruct(*shape) for shape in shapes],
            in_specs=[hbm] * 4,
            out_specs=[hbm, hbm, vmem] + [hbm] * 5,
            scratch_shapes=[
                pltpu.VMEM((LAYERS, 2, own_items, dim), BF16), pltpu.VMEM((2, dim, own_items), F32),
                pltpu.VMEM((LAYERS, dim, own_items), F32), pltpu.VMEM((own_items, dim), F32),
                pltpu.VMEM((8, 8, BUILD), F32), pltpu.VMEM((BUILD, LANES), F32), pltpu.VMEM((1, items), F32),
                pltpu.VMEM((8, 8, BUILD), F32), pltpu.VMEM((2, 8, 8, BUILD), F32),
                pltpu.VMEM((8, items), F32), pltpu.VMEM((8, items), F32),
                pltpu.VMEM((2, batch, dim), BF16), pltpu.VMEM((2, batch, dim), BF16), pltpu.VMEM((4, batch, dim), BF16),
                pltpu.VMEM((batch, dim), F32), pltpu.VMEM((8, LANES), F32), pltpu.VMEM((7, 8, LANES), F32),
                pltpu.VMEM((3, batch), jnp.int32), pltpu.VMEM((3, batch, LANES), jnp.int32),
                pltpu.VMEM((2, half, dim), F32), pltpu.VMEM((2, half, dim), F32), pltpu.VMEM((2, half, dim), F32),
                pltpu.VMEM((2, half, dim), BF16), pltpu.VMEM((own_items, dim), BF16), dma((3,)), dma((2, PARTS)),
                dma((LAYERS, 6)), dma((LAYERS, 6)), dma((LAYERS, 6, PARTS)), dma((LAYERS, 6, PARTS)), dma((LAYERS,)), dma((LAYERS,)),
                dma((LAYERS,)), dma((LAYERS,)), dma((3,)), dma((3,)), dma((4,)), dma((4,)), dma((7,)), dma((7,))],
            compiler_params=pltpu.CompilerParams(collective_id=0, has_side_effects=True, vmem_limit_bytes=60 * 1024 * 1024),
        )(mask_blk, user_shard.reshape(2, half, dim), item_shard, triples.T)
        return outs[0].reshape(shard, dim), outs[1], outs[2].reshape(())

    return jax.shard_map(device_program, mesh=mesh, in_specs=(P('row', COL_AXES), P(USER_AXES, None), P(ITEM_AXES, None), P()), out_specs=(P(USER_AXES, None), P(ITEM_AXES, None), P()), check_vma=False)
```

```python
import functools
import itertools
import math
import jax
import jax.numpy as jnp
from jax import lax
from jax.experimental import pallas as pl
from jax.experimental.pallas import tpu as pltpu
from jax.sharding import PartitionSpec as P

LAYERS = 3
USER_AXES = ('row', 'cola', 'colb')
ITEM_AXES = ('cola', 'colb', 'row')
COL_AXES = ('cola', 'colb')
F32 = jnp.float32
BF16 = jnp.bfloat16
CONTRACT_ROWS = (((0,), (0,)), ((), ()))
CONTRACT_COLS = (((1,), (1,)), ((), ()))
BUILD = 256
TILE = 512
CHUNK = 32
PARTS = 4
DEEP = pl.Buffered(4)
OUT = pl.Buffered(2)
LANES = 128


def kernel(dims, mask, user0, item0, triples, user_out, item_out, loss_out, adj, upan, pbuf, precv, sbuf,
           vpan, acc, qrecv, vtot, us, uscol, isc, degu, drecv, degi, degi_recv, sel, selb, selrecv, mine, lsend, lrecv,
           ids, idcol, base, usum, nearv, local_sem,
           ag_send, ag_recv, rs_send, rs_recv, p_send, p_recv, v_send, v_recv, q_send, q_recv, d_send, d_recv, e_send, e_recv, l_send, l_recv):
    half, items, own_items, dim = dims
    x, y, r = lax.axis_index('colb'), lax.axis_index('cola'), lax.axis_index('row')
    to = {'x': {'colb': 1 - x}, 'y': {'cola': 1 - y}, 'r': {'row': 1 - r},
          'xy': {'colb': 1 - x, 'cola': 1 - y}}
    others = [{'cola': 1 - y if dy else y, 'colb': 1 - x if dx else x, 'row': 1 - r if dr else r}
              for dy, dx, dr in itertools.product((0, 1), repeat=3) if dy or dx or dr]
    pending = []
    batch = ids.shape[1]

    def send_to(src, dst, device, send_sem, recv_sem):
        copy = pltpu.make_async_remote_copy(src_ref=src, dst_ref=dst, send_sem=send_sem, recv_sem=recv_sem,
                                            device_id=device, device_id_type=pl.DeviceIdType.MESH)
        copy.start()
        pending.append(copy)
        return copy

    def send(src, dst, direction, send_sem, recv_sem):
        return send_to(src, dst, to[direction], send_sem, recv_sem)

    def finish(copy):
        copy.wait_send()
        pending[:] = [other for other in pending if other is not copy]

    item_in = pltpu.make_async_copy(item0, vpan.at[0, r], local_sem.at[0])
    ids_in = pltpu.make_async_copy(triples, ids, local_sem.at[1])
    item_in.start()
    ids_in.start()
    barrier = pltpu.get_barrier_semaphore()
    for device in others:
        pl.semaphore_signal(barrier, inc=1, device_id=device, device_id_type=pl.DeviceIdType.MESH)
    pl.semaphore_wait(barrier, len(others))

    def own(k, h):
        return user0.at[h] if k == 0 else upan.at[k, 6 + h]

    def gather_start(k):
        return [send(own(k, 0), upan.at[k, 2], 'x', ag_send.at[k, 0], ag_recv.at[k, 0]),
                send(own(k, 1), upan.at[k, 3], 'y', ag_send.at[k, 1], ag_recv.at[k, 1]),
                send(own(k, 0), upan.at[k, 4], 'y', ag_send.at[k, 2], ag_recv.at[k, 2]),
                send(own(k, 1), upan.at[k, 5], 'x', ag_send.at[k, 3], ag_recv.at[k, 3])]

    def gather_forward(k, copies):
        copies[0].wait_recv()
        far0 = send(upan.at[k, 2], upan.at[k, 0], 'y', ag_send.at[k, 4], ag_recv.at[k, 4])
        copies[1].wait_recv()
        far1 = send(upan.at[k, 3], upan.at[k, 1], 'x', ag_send.at[k, 5], ag_recv.at[k, 5])
        return copies[2:] + [far0, far1]

    def wait_all(copies):
        for copy in copies:
            copy.wait_recv()

    gather0 = gather_start(0)
    item_in.wait()
    ids_in.wait()
    item_copy = send(item0, vpan.at[0, r], 'r', v_send.at[0], v_recv.at[0])

    def mask_block(pos, tile):
        h, q = lax.rem(pos, 2), lax.div(pos, 2)
        prim, sec = 1 - lax.div(q, 2), 1 - lax.rem(q, 2)
        dx, dy = prim * (1 - h) + sec * h, sec * (1 - h) + prim * h
        shard = lax.rem(y + dy, 2) * 2 + lax.rem(x + dx, 2)
        return (shard * 2 + h) * (half // BUILD) + tile

    degu[...] = jnp.zeros_like(degu)
    degi[...] = jnp.zeros_like(degi)
    acc[...] = jnp.zeros_like(acc)

    def degree_body(m_ref):
        pos, tile = pl.program_id(0), pl.program_id(1)

        def chunk(i, cols):
            m = m_ref[pl.ds(pl.multiple_of(i * CHUNK, CHUNK), CHUNK), :]
            part = m[:, :LANES]
            for j in range(1, items // LANES):
                part = part + m[:, j * LANES:(j + 1) * LANES]
            uscol[pl.ds(pl.multiple_of(i * CHUNK, CHUNK), CHUNK), :] = part.astype(F32)
            for j in range(CHUNK // 8):
                cols = cols + m[j * 8:(j + 1) * 8, :]
            return cols

        cols = lax.fori_loop(0, BUILD // CHUNK, chunk, jnp.zeros((8, items), jnp.int32))
        degi[...] += cols.astype(F32)
        pick = (lax.broadcasted_iota(jnp.int32, (8, LANES), 0) == tile).astype(BF16)
        degu[pos] += lax.dot_general(pick, uscol[...].astype(BF16), CONTRACT_COLS, preferred_element_type=F32)

    pltpu.emit_pipeline(degree_body, grid=(8, half // BUILD),
                        in_specs=[pl.BlockSpec((BUILD, items), lambda p, t: (mask_block(p, t), 0), pipeline_mode=DEEP)])(mask)
    item_deg = send(degi, degi_recv, 'r', d_send.at[0], d_recv.at[0])
    user_deg = [send(degu, drecv.at[i], direction, d_send.at[1 + i], d_recv.at[1 + i]) for i, direction in enumerate(('x', 'y', 'xy'))]
    rest0 = gather_forward(0, gather0)
    item_deg.wait_recv()
    total = jnp.sum(degi[...] + degi_recv[...], axis=0, keepdims=True)
    isc[...] = lax.rsqrt(jnp.maximum(total, 1.0))
    wait_all(user_deg)
    for pos in range(8):
        flips = (2, 4, 6) if pos % 2 else (4, 2, 6)
        count = (degu[pos] + drecv[0, pos ^ flips[0]]) + (drecv[1, pos ^ flips[1]] + drecv[2, pos ^ flips[2]])
        us[pos] = lax.rsqrt(jnp.maximum(count, 1.0))
    item_copy.wait_recv()

    def panel(k):
        return vpan[k].reshape(items, dim)

    def add_items(a_ref, u_ref):
        for j in range(2):
            acc[j] += lax.dot_general(u_ref[...], a_ref[:, j * own_items:(j + 1) * own_items], CONTRACT_ROWS,
                                      preferred_element_type=F32)

    def build(first, count, users, start_tile=0, tiles=half // BUILD):
        def body(m_ref, *refs):
            (u_ref, a_ref, p_ref) = refs if users is not None else (None,) + refs
            pos, tile = pl.program_id(0) + first, pl.program_id(1) + start_tile
            row = us[pos, pl.ds(tile, 1), :]
            uscol[...] = jnp.transpose(jnp.broadcast_to(row, (LANES, BUILD)))

            def chunk(i, carry):
                rows = pl.ds(pl.multiple_of(i * CHUNK, CHUNK), CHUNK)
                scale = uscol[rows, :]
                for j in range(items // LANES):
                    cols = slice(j * LANES, (j + 1) * LANES)
                    weight = (scale * m_ref[rows, cols].astype(F32)) * isc[:, cols]
                    a_ref[rows, cols] = weight.astype(BF16)
                return carry

            lax.fori_loop(0, BUILD // CHUNK, chunk, 0)
            p_ref[...] = jnp.dot(a_ref[...], panel(0), preferred_element_type=F32)
            if users is not None:
                add_items(a_ref, u_ref)

        operands = [mask]
        in_specs = [pl.BlockSpec((BUILD, items), lambda p, t: (mask_block(p + first, t + start_tile), 0), pipeline_mode=DEEP)]
        if users is not None:
            ref, start = users
            operands.append(ref)
            in_specs.append(pl.BlockSpec((None, BUILD, dim), lambda p, t: (p + (first - start), t + start_tile, 0), pipeline_mode=DEEP))
        pltpu.emit_pipeline(body, grid=(count, tiles), in_specs=in_specs,
                            out_specs=[pl.BlockSpec((None, BUILD, items), lambda p, t: (p + first, t + start_tile, 0), pipeline_mode=OUT),
                                       pl.BlockSpec((None, BUILD, dim), lambda p, t: (p + first, t + start_tile, 0), pipeline_mode=OUT)])(*operands, adj, pbuf.at[0])

    def multiply(k, first, count):
        def body(a_ref, p_ref):
            p_ref[...] = jnp.dot(a_ref[...], panel(k), preferred_element_type=F32)
        pltpu.emit_pipeline(body, grid=(count, half // TILE),
                            in_specs=[pl.BlockSpec((None, TILE, items), lambda p, t: (p + first, t, 0), pipeline_mode=DEEP)],
                            out_specs=[pl.BlockSpec((None, TILE, dim), lambda p, t: (p + first, t, 0), pipeline_mode=OUT)])(adj, pbuf.at[k])

    def accumulate(k, count):
        pltpu.emit_pipeline(add_items, grid=(count, half // TILE),
                            in_specs=[pl.BlockSpec((None, TILE, items), lambda p, t: (p, t, 0), pipeline_mode=DEEP),
                                      pl.BlockSpec((None, TILE, dim), lambda p, t: (p, t, 0), pipeline_mode=DEEP)])(adj, upan.at[k])

    def scatter_send(k, pos, part=0, parts=1):
        rows = pl.ds(part * (half // parts), half // parts)
        last = k == LAYERS - 1 and pos >= 2
        dst = nearv.at[pos - 2, rows] if last else precv.at[k, pos, rows]
        index = (pos - 2) * PARTS + part if last else 2 * PARTS + part - 1
        sems = (rs_send.at[k, pos], rs_recv.at[k, pos]) if part == 0 and not last else (p_send.at[index], p_recv.at[index])
        return send(pbuf.at[k, pos, rows], dst, 'y' if pos % 2 else 'x', *sems)

    tile_spec = pl.BlockSpec((TILE, dim), lambda t: (t, 0), pipeline_mode=DEEP)
    out_spec = pl.BlockSpec((TILE, dim), lambda t: (t, 0), pipeline_mode=OUT)

    def scatter_last(k, h, far):
        wait_all(far)

        def body(p_ref, r_ref, s_ref):
            s_ref[...] = p_ref[...] + r_ref[...]
        pltpu.emit_pipeline(body, grid=(half // TILE,), in_specs=[tile_spec] * 2, out_specs=[out_spec])(
            pbuf.at[k, 4 + h], precv.at[k, h], sbuf.at[k, h])
        return send(sbuf.at[k, h], precv.at[k, 4 + h], 'x' if h else 'y', rs_send.at[k, 4 + h], rs_recv.at[k, 4 + h])

    def scatter_finish(k, h, near, last):
        near.wait_recv()
        last.wait_recv()

        def body(p_ref, n_ref, l_ref, u_ref):
            u_ref[...] = ((p_ref[...] + n_ref[...]) + l_ref[...]).astype(BF16)
        pltpu.emit_pipeline(body, grid=(half // TILE,), in_specs=[tile_spec] * 3, out_specs=[out_spec])(
            pbuf.at[k, 6 + h], precv.at[k, 2 + h], precv.at[k, 4 + h], upan.at[k + 1, 6 + h])

    def item_layer(k):
        copy = send(acc.at[1 - r], qrecv.at[k - 1], 'r', q_send.at[k - 1], q_recv.at[k - 1])
        copy.wait_recv()
        rows = jnp.transpose(acc[r] + qrecv[k - 1]).astype(BF16)
        vtot[...] += rows.astype(F32)
        finish(copy)
        if k < LAYERS:
            vpan[k, r] = rows
            other = send(vpan.at[k, r], vpan.at[k, r], 'r', v_send.at[k], v_recv.at[k])
            acc[...] = jnp.zeros_like(acc)
            other.wait_recv()

    vtot[...] = vpan[0, r].astype(F32)
    for j in range(3):
        row = jnp.broadcast_to(ids[j:j + 1, :].astype(F32), (LANES, batch))
        idcol[j] = jnp.transpose(row).astype(jnp.int32)
    far, near = {}, {}
    build(0, 1, None)
    far[0, 0] = [scatter_send(0, 0)]
    far[0, 1] = []
    for part in range(2):
        build(1, 1, None, part * (half // BUILD // 2), half // BUILD // 2)
        far[0, 1].append(scatter_send(0, 1, part, 2))
    build(2, 1, (upan.at[0], 0))
    near[0, 0] = scatter_send(0, 2)
    build(3, 1, (upan.at[0], 0))
    near[0, 1] = scatter_send(0, 3)
    wait_all(rest0[:2])
    build(4, 2, (upan.at[0], 0))
    build(6, 2, (user0, 6))
    wait_all(rest0[2:])
    last0 = [scatter_last(0, h, far[0, h]) for h in (0, 1)]
    accumulate(0, 2)
    item_layer(1)
    for pos in range(2):
        multiply(1, pos, 1)
        far[1, pos] = [scatter_send(1, pos)]
    multiply(1, 2, 6)
    for h in (0, 1):
        scatter_finish(0, h, near[0, h], last0[h])
    gather1 = gather_start(1)
    rest1 = gather_forward(1, gather1)
    for pos in (2, 3):
        near[1, pos % 2] = scatter_send(1, pos)
    last1 = [scatter_last(1, h, far[1, h]) for h in (0, 1)]
    wait_all(rest1)
    accumulate(1, 8)
    item_layer(2)
    for pos in range(2):
        multiply(2, pos, 1)
        far[2, pos] = [scatter_send(2, pos)]
    multiply(2, 2, 6)
    for h in (0, 1):
        scatter_finish(1, h, near[1, h], last1[h])
    gather2 = gather_start(2)
    rest2 = gather_forward(2, gather2)
    last2 = [scatter_last(2, h, far[2, h]) for h in (0, 1)]
    wait_all(rest2)
    accumulate(2, 8)
    item_layer(3)

    out_rows = (vtot[...] / (LAYERS + 1)).astype(BF16)
    item_out[...] = out_rows
    item_base = ((y * 2 + x) * 2 + r) * own_items
    for j in range(2):
        hit = (idcol[1 + j, :, 0:1] - item_base) == lax.broadcasted_iota(jnp.int32, (batch, own_items), 1)
        selb[j] = jnp.dot(hit.astype(BF16), out_rows, preferred_element_type=F32).astype(BF16)
    core = send(selb.at[1 - r], selrecv.at[0], 'r', e_send.at[0], e_recv.at[0])
    core.wait_recv()
    sel[0] = selb[r] + selrecv[0]
    xrow = send(sel.at[0], selrecv.at[1], 'x', e_send.at[1], e_recv.at[1])
    parts = {2: [scatter_send(2, 2, 0, PARTS)], 3: [scatter_send(2, 3, 0, PARTS)]}
    xrow.wait_recv()
    sel[1] = sel[0] + selrecv[1]
    yrow = send(sel.at[1], selrecv.at[2], 'y', e_send.at[2], e_recv.at[2])
    for part in range(1, PARTS):
        for pos in (2, 3):
            parts[pos].append(scatter_send(2, pos, part, PARTS))

    for h in (0, 1):
        last2[h].wait_recv()

        def body(p_ref, l_ref, u0_ref, u1_ref, u2_ref, h=h):
            rows = pl.ds(pl.multiple_of(pl.program_id(0) * TILE, TILE), TILE)
            base[h, rows, :] = p_ref[...] + l_ref[...]
            usum[h, rows, :] = (u0_ref[...].astype(F32) + u1_ref[...].astype(F32)) + u2_ref[...].astype(F32)
        pltpu.emit_pipeline(body, grid=(half // TILE,), in_specs=[tile_spec] * 5)(
            pbuf.at[2, 6 + h], precv.at[2, 4 + h], user0.at[h], upan.at[1, 6 + h], upan.at[2, 6 + h])
    yrow.wait_recv()
    finish(core)
    selb[r] = sel[1] + selrecv[2]
    back = send(selb.at[r], selrecv.at[3], 'r', e_send.at[3], e_recv.at[3])
    back.wait_recv()

    user_base = ((r * 2 + y) * 2 + x) * (2 * half)
    local = idcol[0, :, 0:1] - user_base
    mine[...] = jnp.zeros_like(mine)
    size = half // PARTS
    for part in range(PARTS):
        rows = pl.ds(part * size, size)
        for h in (0, 1):
            parts[2 + h][part].wait_recv()
            last_user = (base[h, rows, :] + nearv[h, rows, :]).astype(BF16)
            mean = ((usum[h, rows, :] + last_user.astype(F32)) / (LAYERS + 1)).astype(BF16)
            user_out[h, rows, :] = mean
            hit = (local - (h * half + part * size)) == lax.broadcasted_iota(jnp.int32, (batch, size), 1)
            mine[...] += jnp.dot(hit.astype(BF16), mean, preferred_element_type=F32)
    own_rows, other_rows = selb[r].astype(F32), selrecv[3].astype(F32)
    pos_rows = jnp.where(r == 0, own_rows, other_rows)
    neg_rows = jnp.where(r == 0, other_rows, own_rows)
    rows = mine[...]
    margin = (jnp.sum(rows * pos_rows, axis=1, keepdims=True) - jnp.sum(rows * neg_rows, axis=1, keepdims=True)) / math.sqrt(dim)
    soft = jnp.maximum(-margin, 0.0) + jnp.log1p(jnp.exp(-jnp.abs(margin)))
    terms = jnp.where((local >= 0) & (local < 2 * half), soft, 0.0)
    lsend[...] = jnp.broadcast_to(jnp.sum(terms, axis=0, keepdims=True), (8, LANES))
    shared = [send_to(lsend, lrecv.at[i], device, l_send.at[i], l_recv.at[i]) for i, device in enumerate(others)]
    for copy in pending:
        copy.wait_send()
    wait_all(shared)
    level = [lsend[...]] + [lrecv[i] for i in range(len(others))]
    while len(level) > 1:
        level = [level[i] + level[i + 1] for i in range(0, len(level), 2)]
    loss_out[...] = level[0][0:1, 0:1] / batch


def solution(mesh):
    def device_program(mask_blk, user_shard, item_shard, triples):
        shard, dim = user_shard.shape
        half, items, own_items, batch = shard // 2, mask_blk.shape[1], item_shard.shape[0], triples.shape[0]
        hbm = pl.BlockSpec(memory_space=pltpu.HBM)
        vmem = pl.BlockSpec(memory_space=pltpu.VMEM)
        shapes = [((2, half, dim), BF16), ((own_items, dim), BF16), ((1, 1), F32), ((8, half, items), BF16),
                  ((LAYERS, 8, half, dim), BF16), ((LAYERS, 8, half, dim), F32), ((LAYERS, 6, half, dim), F32),
                  ((LAYERS, 2, half, dim), F32)]
        dma = pltpu.SemaphoreType.DMA
        outs = pl.pallas_call(
            functools.partial(kernel, (half, items, own_items, dim)),
            out_shape=[jax.ShapeDtypeStruct(*shape) for shape in shapes],
            in_specs=[hbm] * 4,
            out_specs=[vmem, vmem, vmem] + [hbm] * 5,
            scratch_shapes=[
                pltpu.VMEM((LAYERS, 2, own_items, dim), BF16), pltpu.VMEM((2, dim, own_items), F32),
                pltpu.VMEM((LAYERS, dim, own_items), F32), pltpu.VMEM((own_items, dim), F32),
                pltpu.VMEM((8, 8, BUILD), F32), pltpu.VMEM((BUILD, LANES), F32), pltpu.VMEM((1, items), F32),
                pltpu.VMEM((8, 8, BUILD), F32), pltpu.VMEM((3, 8, 8, BUILD), F32),
                pltpu.VMEM((8, items), F32), pltpu.VMEM((8, items), F32),
                pltpu.VMEM((2, batch, dim), BF16), pltpu.VMEM((2, batch, dim), BF16), pltpu.VMEM((4, batch, dim), BF16),
                pltpu.VMEM((batch, dim), F32), pltpu.VMEM((8, LANES), F32), pltpu.VMEM((7, 8, LANES), F32),
                pltpu.VMEM((3, batch), jnp.int32), pltpu.VMEM((3, batch, LANES), jnp.int32),
                pltpu.VMEM((2, half, dim), F32), pltpu.VMEM((2, half, dim), F32), pltpu.VMEM((2, half, dim), F32),
                dma((2,)),
                dma((LAYERS, 6)), dma((LAYERS, 6)), dma((LAYERS, 6)), dma((LAYERS, 6)), dma((2 * PARTS + 1,)), dma((2 * PARTS + 1,)), dma((LAYERS,)), dma((LAYERS,)),
                dma((LAYERS,)), dma((LAYERS,)), dma((4,)), dma((4,)), dma((4,)), dma((4,)), dma((7,)), dma((7,))],
            compiler_params=pltpu.CompilerParams(collective_id=0, has_side_effects=True, vmem_limit_bytes=48 * 1024 * 1024),
        )(*[pltpu.with_memory_space_constraint(a, pltpu.HBM) for a in (mask_blk, user_shard.reshape(2, half, dim), item_shard, triples.T)])
        return outs[0].reshape(shard, dim), outs[1], outs[2].reshape(())

    return jax.shard_map(device_program, mesh=mesh, in_specs=(P('row', COL_AXES), P(USER_AXES, None), P(ITEM_AXES, None), P()), out_specs=(P(USER_AXES, None), P(ITEM_AXES, None), P()), check_vma=False)
```

```python
import functools
import itertools
import math
import jax
import jax.numpy as jnp
from jax import lax
from jax.experimental import pallas as pl
from jax.experimental.pallas import tpu as pltpu
from jax.sharding import PartitionSpec as P

LAYERS = 3
USER_AXES = ('row', 'cola', 'colb')
ITEM_AXES = ('cola', 'colb', 'row')
COL_AXES = ('cola', 'colb')
F32 = jnp.float32
BF16 = jnp.bfloat16
CONTRACT_ROWS = (((0,), (0,)), ((), ()))
CONTRACT_COLS = (((1,), (1,)), ((), ()))
BUILD = 256
TILE = 512
CHUNK = 32
PARTS = 4
DEEP = pl.Buffered(4)
OUT = pl.Buffered(2)
LANES = 128


def kernel(dims, mask, user0, item0, triples, user_out, item_out, loss_out, adj, upan, pbuf, precv, sbuf,
           vpan, acc, qrecv, vtot, us, uscol, isc, degu, dsend, drecv, degi, degi_recv, sel, selb, selrecv, mine, lsend, lrecv,
           ids, idcol, base, usum, nearv, local_sem,
           ag_send, ag_recv, rs_send, rs_recv, p_send, p_recv, v_send, v_recv, q_send, q_recv, d_send, d_recv, e_send, e_recv, l_send, l_recv):
    half, items, own_items, dim = dims
    x, y, r = lax.axis_index('colb'), lax.axis_index('cola'), lax.axis_index('row')
    to = {'x': {'colb': 1 - x}, 'y': {'cola': 1 - y}, 'r': {'row': 1 - r},
          'xy': {'colb': 1 - x, 'cola': 1 - y}}
    others = [{'cola': 1 - y if dy else y, 'colb': 1 - x if dx else x, 'row': 1 - r if dr else r}
              for dy, dx, dr in itertools.product((0, 1), repeat=3) if dy or dx or dr]
    pending = []
    batch = ids.shape[1]

    def send_to(src, dst, device, send_sem, recv_sem):
        copy = pltpu.make_async_remote_copy(src_ref=src, dst_ref=dst, send_sem=send_sem, recv_sem=recv_sem,
                                            device_id=device, device_id_type=pl.DeviceIdType.MESH)
        copy.start()
        pending.append(copy)
        return copy

    def send(src, dst, direction, send_sem, recv_sem):
        return send_to(src, dst, to[direction], send_sem, recv_sem)

    def finish(copy):
        copy.wait_send()
        pending[:] = [other for other in pending if other is not copy]

    item_in = pltpu.make_async_copy(item0, vpan.at[0, r], local_sem.at[0])
    ids_in = pltpu.make_async_copy(triples, ids, local_sem.at[1])
    item_in.start()
    ids_in.start()
    barrier = pltpu.get_barrier_semaphore()
    for device in others:
        pl.semaphore_signal(barrier, inc=1, device_id=device, device_id_type=pl.DeviceIdType.MESH)
    pl.semaphore_wait(barrier, len(others))

    def own(k, h):
        return user0.at[h] if k == 0 else upan.at[k, 6 + h]

    def gather_start(k):
        return [send(own(k, 0), upan.at[k, 2], 'x', ag_send.at[k, 0], ag_recv.at[k, 0]),
                send(own(k, 1), upan.at[k, 3], 'y', ag_send.at[k, 1], ag_recv.at[k, 1]),
                send(own(k, 0), upan.at[k, 4], 'y', ag_send.at[k, 2], ag_recv.at[k, 2]),
                send(own(k, 1), upan.at[k, 5], 'x', ag_send.at[k, 3], ag_recv.at[k, 3])]

    def gather_forward(k, copies):
        copies[0].wait_recv()
        far0 = send(upan.at[k, 2], upan.at[k, 0], 'y', ag_send.at[k, 4], ag_recv.at[k, 4])
        copies[1].wait_recv()
        far1 = send(upan.at[k, 3], upan.at[k, 1], 'x', ag_send.at[k, 5], ag_recv.at[k, 5])
        return copies[2:] + [far0, far1]

    def wait_all(copies):
        for copy in copies:
            copy.wait_recv()

    gather0 = gather_start(0)
    item_in.wait()
    ids_in.wait()
    item_copy = send(item0, vpan.at[0, r], 'r', v_send.at[0], v_recv.at[0])

    def mask_block(pos, tile):
        h, q = lax.rem(pos, 2), lax.div(pos, 2)
        prim, sec = 1 - lax.div(q, 2), 1 - lax.rem(q, 2)
        dx, dy = prim * (1 - h) + sec * h, sec * (1 - h) + prim * h
        shard = lax.rem(y + dy, 2) * 2 + lax.rem(x + dx, 2)
        return (shard * 2 + h) * (half // BUILD) + tile

    degu[...] = jnp.zeros_like(degu)
    degi[...] = jnp.zeros_like(degi)
    acc[...] = jnp.zeros_like(acc)

    def degree_body(m_ref):
        pos, tile = pl.program_id(0), pl.program_id(1)

        def chunk(i, cols):
            m = m_ref[pl.ds(pl.multiple_of(i * CHUNK, CHUNK), CHUNK), :]
            part = m[:, :LANES]
            for j in range(1, items // LANES):
                part = part + m[:, j * LANES:(j + 1) * LANES]
            uscol[pl.ds(pl.multiple_of(i * CHUNK, CHUNK), CHUNK), :] = part.astype(F32)
            for j in range(CHUNK // 8):
                cols = cols + m[j * 8:(j + 1) * 8, :]
            return cols

        cols = lax.fori_loop(0, BUILD // CHUNK, chunk, jnp.zeros((8, items), jnp.int32))
        degi[...] += cols.astype(F32)
        pick = (lax.broadcasted_iota(jnp.int32, (8, LANES), 0) == tile).astype(BF16)
        degu[pos] += lax.dot_general(pick, uscol[...].astype(BF16), CONTRACT_COLS, preferred_element_type=F32)

    pltpu.emit_pipeline(degree_body, grid=(8, half // BUILD),
                        in_specs=[pl.BlockSpec((BUILD, items), lambda p, t: (mask_block(p, t), 0), pipeline_mode=DEEP)])(mask)
    item_deg = send(degi, degi_recv, 'r', d_send.at[0], d_recv.at[0])
    for q in range(4):
        pair = jnp.concatenate([degu[2 * q], degu[2 * q + 1]], axis=0)
        dsend[q] = pair.astype(jnp.int32).astype(jnp.int16)
    user_deg = [send(dsend, drecv.at[i], direction, d_send.at[1 + i], d_recv.at[1 + i]) for i, direction in enumerate(('x', 'y', 'xy'))]
    rest0 = gather_forward(0, gather0)
    item_deg.wait_recv()
    total = jnp.sum(degi[...] + degi_recv[...], axis=0, keepdims=True)
    isc[...] = lax.rsqrt(jnp.maximum(total, 1.0))
    wait_all(user_deg)
    for pos in range(8):
        count = degu[pos]
        for i, flip in enumerate((2, 4, 6) if pos % 2 else (4, 2, 6)):
            part = drecv[i, (pos ^ flip) // 2].astype(jnp.int32)
            count = count + part[pos % 2 * 8:pos % 2 * 8 + 8].astype(F32)
        us[pos] = lax.rsqrt(jnp.maximum(count, 1.0))
    item_copy.wait_recv()

    def panel(k):
        return vpan[k].reshape(items, dim)

    def add_items(a_ref, u_ref):
        for j in range(2):
            acc[j] += lax.dot_general(u_ref[...], a_ref[:, j * own_items:(j + 1) * own_items], CONTRACT_ROWS,
                                      preferred_element_type=F32)

    def build(first, count, users, start_tile=0, tiles=half // BUILD):
        def body(m_ref, *refs):
            (u_ref, a_ref, p_ref) = refs if users is not None else (None,) + refs
            pos, tile = pl.program_id(0) + first, pl.program_id(1) + start_tile
            row = us[pos, pl.ds(tile, 1), :]
            uscol[...] = jnp.transpose(jnp.broadcast_to(row, (LANES, BUILD)))

            def chunk(i, carry):
                rows = pl.ds(pl.multiple_of(i * CHUNK, CHUNK), CHUNK)
                scale = uscol[rows, :]
                for j in range(items // LANES):
                    cols = slice(j * LANES, (j + 1) * LANES)
                    weight = (scale * m_ref[rows, cols].astype(F32)) * isc[:, cols]
                    a_ref[rows, cols] = weight.astype(BF16)
                return carry

            lax.fori_loop(0, BUILD // CHUNK, chunk, 0)
            p_ref[...] = jnp.dot(a_ref[...], panel(0), preferred_element_type=F32)
            if users is not None:
                add_items(a_ref, u_ref)

        operands = [mask]
        in_specs = [pl.BlockSpec((BUILD, items), lambda p, t: (mask_block(p + first, t + start_tile), 0), pipeline_mode=DEEP)]
        if users is not None:
            ref, start = users
            operands.append(ref)
            in_specs.append(pl.BlockSpec((None, BUILD, dim), lambda p, t: (p + (first - start), t + start_tile, 0), pipeline_mode=DEEP))
        pltpu.emit_pipeline(body, grid=(count, tiles), in_specs=in_specs,
                            out_specs=[pl.BlockSpec((None, BUILD, items), lambda p, t: (p + first, t + start_tile, 0), pipeline_mode=OUT),
                                       pl.BlockSpec((None, BUILD, dim), lambda p, t: (p + first, t + start_tile, 0), pipeline_mode=OUT)])(*operands, adj, pbuf.at[0])

    def multiply(k, first, count):
        def body(a_ref, p_ref):
            p_ref[...] = jnp.dot(a_ref[...], panel(k), preferred_element_type=F32)
        pltpu.emit_pipeline(body, grid=(count, half // TILE),
                            in_specs=[pl.BlockSpec((None, TILE, items), lambda p, t: (p + first, t, 0), pipeline_mode=DEEP)],
                            out_specs=[pl.BlockSpec((None, TILE, dim), lambda p, t: (p + first, t, 0), pipeline_mode=OUT)])(adj, pbuf.at[k])

    def accumulate(k, count):
        pltpu.emit_pipeline(add_items, grid=(count, half // TILE),
                            in_specs=[pl.BlockSpec((None, TILE, items), lambda p, t: (p, t, 0), pipeline_mode=DEEP),
                                      pl.BlockSpec((None, TILE, dim), lambda p, t: (p, t, 0), pipeline_mode=DEEP)])(adj, upan.at[k])

    def scatter_send(k, pos, part=0, parts=1):
        rows = pl.ds(part * (half // parts), half // parts)
        last = k == LAYERS - 1 and pos >= 2
        dst = nearv.at[pos - 2, rows] if last else precv.at[k, pos, rows]
        index = (pos - 2) * PARTS + part if last else 2 * PARTS + part - 1
        sems = (rs_send.at[k, pos], rs_recv.at[k, pos]) if part == 0 and not last else (p_send.at[index], p_recv.at[index])
        return send(pbuf.at[k, pos, rows], dst, 'y' if pos % 2 else 'x', *sems)

    tile_spec = pl.BlockSpec((TILE, dim), lambda t: (t, 0), pipeline_mode=DEEP)
    out_spec = pl.BlockSpec((TILE, dim), lambda t: (t, 0), pipeline_mode=OUT)

    def scatter_last(k, h, far):
        wait_all(far)

        def body(p_ref, r_ref, s_ref):
            s_ref[...] = p_ref[...] + r_ref[...]
        pltpu.emit_pipeline(body, grid=(half // TILE,), in_specs=[tile_spec] * 2, out_specs=[out_spec])(
            pbuf.at[k, 4 + h], precv.at[k, h], sbuf.at[k, h])
        return send(sbuf.at[k, h], precv.at[k, 4 + h], 'x' if h else 'y', rs_send.at[k, 4 + h], rs_recv.at[k, 4 + h])

    def scatter_finish(k, h, near, last):
        near.wait_recv()
        last.wait_recv()

        def body(p_ref, n_ref, l_ref, u_ref):
            u_ref[...] = ((p_ref[...] + n_ref[...]) + l_ref[...]).astype(BF16)
        pltpu.emit_pipeline(body, grid=(half // TILE,), in_specs=[tile_spec] * 3, out_specs=[out_spec])(
            pbuf.at[k, 6 + h], precv.at[k, 2 + h], precv.at[k, 4 + h], upan.at[k + 1, 6 + h])

    def item_layer(k):
        copy = send(acc.at[1 - r], qrecv.at[k - 1], 'r', q_send.at[k - 1], q_recv.at[k - 1])
        copy.wait_recv()
        rows = jnp.transpose(acc[r] + qrecv[k - 1]).astype(BF16)
        vtot[...] += rows.astype(F32)
        finish(copy)
        if k < LAYERS:
            vpan[k, r] = rows
            other = send(vpan.at[k, r], vpan.at[k, r], 'r', v_send.at[k], v_recv.at[k])
            acc[...] = jnp.zeros_like(acc)
            other.wait_recv()

    vtot[...] = vpan[0, r].astype(F32)
    for j in range(3):
        row = jnp.broadcast_to(ids[j:j + 1, :].astype(F32), (LANES, batch))
        idcol[j] = jnp.transpose(row).astype(jnp.int32)
    far, near = {}, {}
    build(0, 1, None)
    far[0, 0] = [scatter_send(0, 0)]
    far[0, 1] = []
    for part in range(2):
        build(1, 1, None, part * (half // BUILD // 2), half // BUILD // 2)
        far[0, 1].append(scatter_send(0, 1, part, 2))
    build(2, 1, (upan.at[0], 0))
    near[0, 0] = scatter_send(0, 2)
    build(3, 1, (upan.at[0], 0))
    near[0, 1] = scatter_send(0, 3)
    wait_all(rest0[:2])
    build(4, 2, (upan.at[0], 0))
    build(6, 2, (user0, 6))
    wait_all(rest0[2:])
    last0 = [scatter_last(0, h, far[0, h]) for h in (0, 1)]
    accumulate(0, 2)
    item_layer(1)
    for pos in range(2):
        multiply(1, pos, 1)
        far[1, pos] = [scatter_send(1, pos)]
    multiply(1, 2, 6)
    for h in (0, 1):
        scatter_finish(0, h, near[0, h], last0[h])
    gather1 = gather_start(1)
    rest1 = gather_forward(1, gather1)
    for pos in (2, 3):
        near[1, pos % 2] = scatter_send(1, pos)
    last1 = [scatter_last(1, h, far[1, h]) for h in (0, 1)]
    wait_all(rest1)
    accumulate(1, 8)
    item_layer(2)
    for pos in range(2):
        multiply(2, pos, 1)
        far[2, pos] = [scatter_send(2, pos)]
    multiply(2, 2, 6)
    for h in (0, 1):
        scatter_finish(1, h, near[1, h], last1[h])
    gather2 = gather_start(2)
    rest2 = gather_forward(2, gather2)
    last2 = [scatter_last(2, h, far[2, h]) for h in (0, 1)]
    wait_all(rest2)
    accumulate(2, 8)
    item_layer(3)

    out_rows = (vtot[...] / (LAYERS + 1)).astype(BF16)
    item_out[...] = out_rows
    item_base = ((y * 2 + x) * 2 + r) * own_items
    for j in range(2):
        hit = (idcol[1 + j, :, 0:1] - item_base) == lax.broadcasted_iota(jnp.int32, (batch, own_items), 1)
        selb[j] = jnp.dot(hit.astype(BF16), out_rows, preferred_element_type=F32).astype(BF16)
    core = send(selb.at[1 - r], selrecv.at[0], 'r', e_send.at[0], e_recv.at[0])
    core.wait_recv()
    sel[0] = selb[r] + selrecv[0]
    xrow = send(sel.at[0], selrecv.at[1], 'x', e_send.at[1], e_recv.at[1])
    parts = {2: [scatter_send(2, 2, 0, PARTS)], 3: [scatter_send(2, 3, 0, PARTS)]}
    xrow.wait_recv()
    sel[1] = sel[0] + selrecv[1]
    yrow = send(sel.at[1], selrecv.at[2], 'y', e_send.at[2], e_recv.at[2])
    for part in range(1, PARTS):
        for pos in (2, 3):
            parts[pos].append(scatter_send(2, pos, part, PARTS))

    for h in (0, 1):
        last2[h].wait_recv()

        def body(p_ref, l_ref, u0_ref, u1_ref, u2_ref, h=h):
            rows = pl.ds(pl.multiple_of(pl.program_id(0) * TILE, TILE), TILE)
            base[h, rows, :] = p_ref[...] + l_ref[...]
            usum[h, rows, :] = (u0_ref[...].astype(F32) + u1_ref[...].astype(F32)) + u2_ref[...].astype(F32)
        pltpu.emit_pipeline(body, grid=(half // TILE,), in_specs=[tile_spec] * 5)(
            pbuf.at[2, 6 + h], precv.at[2, 4 + h], user0.at[h], upan.at[1, 6 + h], upan.at[2, 6 + h])
    yrow.wait_recv()
    finish(core)
    selb[r] = sel[1] + selrecv[2]
    back = send(selb.at[r], selrecv.at[3], 'r', e_send.at[3], e_recv.at[3])
    back.wait_recv()

    user_base = ((r * 2 + y) * 2 + x) * (2 * half)
    local = idcol[0, :, 0:1] - user_base
    mine[...] = jnp.zeros_like(mine)
    size = half // PARTS
    for part in range(PARTS):
        rows = pl.ds(part * size, size)
        for h in (0, 1):
            parts[2 + h][part].wait_recv()
            last_user = (base[h, rows, :] + nearv[h, rows, :]).astype(BF16)
            mean = ((usum[h, rows, :] + last_user.astype(F32)) / (LAYERS + 1)).astype(BF16)
            user_out[h, rows, :] = mean
            hit = (local - (h * half + part * size)) == lax.broadcasted_iota(jnp.int32, (batch, size), 1)
            mine[...] += jnp.dot(hit.astype(BF16), mean, preferred_element_type=F32)
    own_rows, other_rows = selb[r].astype(F32), selrecv[3].astype(F32)
    pos_rows = jnp.where(r == 0, own_rows, other_rows)
    neg_rows = jnp.where(r == 0, other_rows, own_rows)
    rows = mine[...]
    margin = (jnp.sum(rows * pos_rows, axis=1, keepdims=True) - jnp.sum(rows * neg_rows, axis=1, keepdims=True)) / math.sqrt(dim)
    soft = jnp.maximum(-margin, 0.0) + jnp.log1p(jnp.exp(-jnp.abs(margin)))
    terms = jnp.where((local >= 0) & (local < 2 * half), soft, 0.0)
    lsend[...] = jnp.broadcast_to(jnp.sum(terms, axis=0, keepdims=True), (8, LANES))
    shared = [send_to(lsend, lrecv.at[i], device, l_send.at[i], l_recv.at[i]) for i, device in enumerate(others)]
    for copy in pending:
        copy.wait_send()
    wait_all(shared)
    level = [lsend[...]] + [lrecv[i] for i in range(len(others))]
    while len(level) > 1:
        level = [level[i] + level[i + 1] for i in range(0, len(level), 2)]
    loss_out[...] = level[0][0:1, 0:1] / batch


def solution(mesh):
    def device_program(mask_blk, user_shard, item_shard, triples):
        shard, dim = user_shard.shape
        half, items, own_items, batch = shard // 2, mask_blk.shape[1], item_shard.shape[0], triples.shape[0]
        hbm = pl.BlockSpec(memory_space=pltpu.HBM)
        vmem = pl.BlockSpec(memory_space=pltpu.VMEM)
        shapes = [((2, half, dim), BF16), ((own_items, dim), BF16), ((1, 1), F32), ((8, half, items), BF16),
                  ((LAYERS, 8, half, dim), BF16), ((LAYERS, 8, half, dim), F32), ((LAYERS, 6, half, dim), F32),
                  ((LAYERS, 2, half, dim), F32)]
        dma = pltpu.SemaphoreType.DMA
        outs = pl.pallas_call(
            functools.partial(kernel, (half, items, own_items, dim)),
            out_shape=[jax.ShapeDtypeStruct(*shape) for shape in shapes],
            in_specs=[hbm] * 4,
            out_specs=[vmem, vmem, vmem] + [hbm] * 5,
            scratch_shapes=[
                pltpu.VMEM((LAYERS, 2, own_items, dim), BF16), pltpu.VMEM((2, dim, own_items), F32),
                pltpu.VMEM((LAYERS, dim, own_items), F32), pltpu.VMEM((own_items, dim), F32),
                pltpu.VMEM((8, 8, BUILD), F32), pltpu.VMEM((BUILD, LANES), F32), pltpu.VMEM((1, items), F32),
                pltpu.VMEM((8, 8, BUILD), F32), pltpu.VMEM((4, 16, BUILD), jnp.int16), pltpu.VMEM((3, 4, 16, BUILD), jnp.int16),
                pltpu.VMEM((8, items), F32), pltpu.VMEM((8, items), F32),
                pltpu.VMEM((2, batch, dim), BF16), pltpu.VMEM((2, batch, dim), BF16), pltpu.VMEM((4, batch, dim), BF16),
                pltpu.VMEM((batch, dim), F32), pltpu.VMEM((8, LANES), F32), pltpu.VMEM((7, 8, LANES), F32),
                pltpu.VMEM((3, batch), jnp.int32), pltpu.VMEM((3, batch, LANES), jnp.int32),
                pltpu.VMEM((2, half, dim), F32), pltpu.VMEM((2, half, dim), F32), pltpu.VMEM((2, half, dim), F32),
                dma((2,)),
                dma((LAYERS, 6)), dma((LAYERS, 6)), dma((LAYERS, 6)), dma((LAYERS, 6)), dma((2 * PARTS + 1,)), dma((2 * PARTS + 1,)), dma((LAYERS,)), dma((LAYERS,)),
                dma((LAYERS,)), dma((LAYERS,)), dma((4,)), dma((4,)), dma((4,)), dma((4,)), dma((7,)), dma((7,))],
            compiler_params=pltpu.CompilerParams(collective_id=0, has_side_effects=True, vmem_limit_bytes=48 * 1024 * 1024),
        )(*[pltpu.with_memory_space_constraint(a, pltpu.HBM) for a in (mask_blk, user_shard.reshape(2, half, dim), item_shard, triples.T)])
        return outs[0].reshape(shard, dim), outs[1], outs[2].reshape(())

    return jax.shard_map(device_program, mesh=mesh, in_specs=(P('row', COL_AXES), P(USER_AXES, None), P(ITEM_AXES, None), P()), out_specs=(P(USER_AXES, None), P(ITEM_AXES, None), P()), check_vma=False)
```

```python
import functools
import itertools
import math
import jax
import jax.numpy as jnp
from jax import lax
from jax.experimental import pallas as pl
from jax.experimental.pallas import tpu as pltpu
from jax.sharding import PartitionSpec as P

LAYERS = 3
USER_AXES = ('row', 'cola', 'colb')
ITEM_AXES = ('cola', 'colb', 'row')
COL_AXES = ('cola', 'colb')
F32 = jnp.float32
BF16 = jnp.bfloat16
CONTRACT_ROWS = (((0,), (0,)), ((), ()))
CONTRACT_COLS = (((1,), (1,)), ((), ()))
BUILD = 256
TILE = 512
CHUNK = 32
PARTS = 4
HEAD = 256
DEEP = pl.Buffered(4)
OUT = pl.Buffered(2)
LANES = 128


def kernel(dims, mask, user0, item0, triples, user_out, item_out, loss_out, adj, upan, pbuf, precv, sbuf,
           vpan, acc, qrecv, vtot, us, uscol, isc, degu, drecv, degi, degi_recv, sel, selb, selrecv, mine, lsend, lrecv,
           ids, idcol, base, usum, nearv, local_sem,
           ag_send, ag_recv, rs_send, rs_recv, p_send, p_recv, v_send, v_recv, q_send, q_recv, d_send, d_recv, e_send, e_recv, l_send, l_recv):
    half, items, own_items, dim = dims
    x, y, r = lax.axis_index('colb'), lax.axis_index('cola'), lax.axis_index('row')
    to = {'x': {'colb': 1 - x}, 'y': {'cola': 1 - y}, 'r': {'row': 1 - r},
          'xy': {'colb': 1 - x, 'cola': 1 - y}}
    others = [{'cola': 1 - y if dy else y, 'colb': 1 - x if dx else x, 'row': 1 - r if dr else r}
              for dy, dx, dr in itertools.product((0, 1), repeat=3) if dy or dx or dr]
    pending = []
    batch = ids.shape[1]

    def send_to(src, dst, device, send_sem, recv_sem):
        copy = pltpu.make_async_remote_copy(src_ref=src, dst_ref=dst, send_sem=send_sem, recv_sem=recv_sem,
                                            device_id=device, device_id_type=pl.DeviceIdType.MESH)
        copy.start()
        pending.append(copy)
        return copy

    def send(src, dst, direction, send_sem, recv_sem):
        return send_to(src, dst, to[direction], send_sem, recv_sem)

    def finish(copy):
        copy.wait_send()
        pending[:] = [other for other in pending if other is not copy]

    item_in = pltpu.make_async_copy(item0, vpan.at[0, r], local_sem.at[0])
    ids_in = pltpu.make_async_copy(triples, ids, local_sem.at[1])
    item_in.start()
    ids_in.start()
    barrier = pltpu.get_barrier_semaphore()
    for device in others:
        pl.semaphore_signal(barrier, inc=1, device_id=device, device_id_type=pl.DeviceIdType.MESH)
    pl.semaphore_wait(barrier, len(others))

    def own(k, h):
        return user0.at[h] if k == 0 else upan.at[k, 6 + h]

    def gather_start(k):
        return [send(own(k, 0), upan.at[k, 2], 'x', ag_send.at[k, 0], ag_recv.at[k, 0]),
                send(own(k, 1), upan.at[k, 3], 'y', ag_send.at[k, 1], ag_recv.at[k, 1]),
                send(own(k, 0), upan.at[k, 4], 'y', ag_send.at[k, 2], ag_recv.at[k, 2]),
                send(own(k, 1), upan.at[k, 5], 'x', ag_send.at[k, 3], ag_recv.at[k, 3])]

    def gather_forward(k, copies):
        copies[0].wait_recv()
        far0 = send(upan.at[k, 2], upan.at[k, 0], 'y', ag_send.at[k, 4], ag_recv.at[k, 4])
        copies[1].wait_recv()
        far1 = send(upan.at[k, 3], upan.at[k, 1], 'x', ag_send.at[k, 5], ag_recv.at[k, 5])
        return copies[2:] + [far0, far1]

    def wait_all(copies):
        for copy in copies:
            copy.wait_recv()

    gather0 = gather_start(0)
    item_in.wait()
    ids_in.wait()
    item_copy = send(item0, vpan.at[0, r], 'r', v_send.at[0], v_recv.at[0])

    def mask_block(pos, tile):
        h, q = lax.rem(pos, 2), lax.div(pos, 2)
        prim, sec = 1 - lax.div(q, 2), 1 - lax.rem(q, 2)
        dx, dy = prim * (1 - h) + sec * h, sec * (1 - h) + prim * h
        shard = lax.rem(y + dy, 2) * 2 + lax.rem(x + dx, 2)
        return (shard * 2 + h) * (half // BUILD) + tile

    degu[...] = jnp.zeros_like(degu)
    degi[...] = jnp.zeros_like(degi)
    acc[...] = jnp.zeros_like(acc)

    def degree_body(m_ref):
        pos, tile = pl.program_id(0), pl.program_id(1)

        def chunk(i, cols):
            m = m_ref[pl.ds(pl.multiple_of(i * CHUNK, CHUNK), CHUNK), :]
            part = m[:, :LANES]
            for j in range(1, items // LANES):
                part = part + m[:, j * LANES:(j + 1) * LANES]
            uscol[pl.ds(pl.multiple_of(i * CHUNK, CHUNK), CHUNK), :] = part.astype(F32)
            for j in range(CHUNK // 8):
                cols = cols + m[j * 8:(j + 1) * 8, :]
            return cols

        cols = lax.fori_loop(0, BUILD // CHUNK, chunk, jnp.zeros((8, items), jnp.int32))
        degi[...] += cols.astype(F32)
        pick = (lax.broadcasted_iota(jnp.int32, (8, LANES), 0) == tile).astype(BF16)
        degu[pos] += lax.dot_general(pick, uscol[...].astype(BF16), CONTRACT_COLS, preferred_element_type=F32)

    pltpu.emit_pipeline(degree_body, grid=(8, half // BUILD),
                        in_specs=[pl.BlockSpec((BUILD, items), lambda p, t: (mask_block(p, t), 0), pipeline_mode=DEEP)])(mask)
    item_deg = send(degi, degi_recv, 'r', d_send.at[0], d_recv.at[0])
    user_deg = send(degu, drecv.at[0], 'x', d_send.at[1], d_recv.at[1])
    head, tail = pl.ds(0, HEAD), pl.ds(HEAD, half - HEAD)
    gather0[0].wait_recv()
    rest0 = gather0[2:] + [send(upan.at[0, 2, head], upan.at[0, 0, head], 'y', ag_send.at[0, 4], ag_recv.at[0, 4])]
    gather0[1].wait_recv()
    rest0.append(send(upan.at[0, 3], upan.at[0, 1], 'x', ag_send.at[0, 5], ag_recv.at[0, 5]))
    user_deg.wait_recv()
    for pos in range(8):
        us[pos] = degu[pos] + drecv[0, pos ^ (2 if pos % 2 else 4)]
    user_deg2 = send(us, drecv.at[1], 'y', d_send.at[2], d_recv.at[2])
    rest0.append(send(upan.at[0, 2, tail], upan.at[0, 0, tail], 'y', d_send.at[3], d_recv.at[3]))
    item_deg.wait_recv()
    total = jnp.sum(degi[...] + degi_recv[...], axis=0, keepdims=True)
    isc[...] = lax.rsqrt(jnp.maximum(total, 1.0))
    user_deg2.wait_recv()
    finish(user_deg)
    for pos in range(8):
        degu[pos] = lax.rsqrt(jnp.maximum(us[pos] + drecv[1, pos ^ (4 if pos % 2 else 2)], 1.0))
    item_copy.wait_recv()

    def panel(k):
        return vpan[k].reshape(items, dim)

    def add_items(a_ref, u_ref):
        for j in range(2):
            acc[j] += lax.dot_general(u_ref[...], a_ref[:, j * own_items:(j + 1) * own_items], CONTRACT_ROWS,
                                      preferred_element_type=F32)

    def build(first, count, users, start_tile=0, tiles=half // BUILD):
        def body(m_ref, *refs):
            (u_ref, a_ref, p_ref) = refs if users is not None else (None,) + refs
            pos, tile = pl.program_id(0) + first, pl.program_id(1) + start_tile
            row = degu[pos, pl.ds(tile, 1), :]
            uscol[...] = jnp.transpose(jnp.broadcast_to(row, (LANES, BUILD)))

            def chunk(i, carry):
                rows = pl.ds(pl.multiple_of(i * CHUNK, CHUNK), CHUNK)
                scale = uscol[rows, :]
                for j in range(items // LANES):
                    cols = slice(j * LANES, (j + 1) * LANES)
                    weight = (scale * m_ref[rows, cols].astype(F32)) * isc[:, cols]
                    a_ref[rows, cols] = weight.astype(BF16)
                return carry

            lax.fori_loop(0, BUILD // CHUNK, chunk, 0)
            p_ref[...] = jnp.dot(a_ref[...], panel(0), preferred_element_type=F32)
            if users is not None:
                add_items(a_ref, u_ref)

        operands = [mask]
        in_specs = [pl.BlockSpec((BUILD, items), lambda p, t: (mask_block(p + first, t + start_tile), 0), pipeline_mode=DEEP)]
        if users is not None:
            ref, start = users
            operands.append(ref)
            in_specs.append(pl.BlockSpec((None, BUILD, dim), lambda p, t: (p + (first - start), t + start_tile, 0), pipeline_mode=DEEP))
        pltpu.emit_pipeline(body, grid=(count, tiles), in_specs=in_specs,
                            out_specs=[pl.BlockSpec((None, BUILD, items), lambda p, t: (p + first, t + start_tile, 0), pipeline_mode=OUT),
                                       pl.BlockSpec((None, BUILD, dim), lambda p, t: (p + first, t + start_tile, 0), pipeline_mode=OUT)])(*operands, adj, pbuf.at[0])

    def multiply(k, first, count):
        def body(a_ref, p_ref):
            p_ref[...] = jnp.dot(a_ref[...], panel(k), preferred_element_type=F32)
        pltpu.emit_pipeline(body, grid=(count, half // TILE),
                            in_specs=[pl.BlockSpec((None, TILE, items), lambda p, t: (p + first, t, 0), pipeline_mode=DEEP)],
                            out_specs=[pl.BlockSpec((None, TILE, dim), lambda p, t: (p + first, t, 0), pipeline_mode=OUT)])(adj, pbuf.at[k])

    def accumulate(k, count):
        pltpu.emit_pipeline(add_items, grid=(count, half // TILE),
                            in_specs=[pl.BlockSpec((None, TILE, items), lambda p, t: (p, t, 0), pipeline_mode=DEEP),
                                      pl.BlockSpec((None, TILE, dim), lambda p, t: (p, t, 0), pipeline_mode=DEEP)])(adj, upan.at[k])

    def scatter_send(k, pos, part=0, parts=1):
        rows = pl.ds(part * (half // parts), half // parts)
        last = k == LAYERS - 1 and pos >= 2
        dst = nearv.at[pos - 2, rows] if last else precv.at[k, pos, rows]
        index = (pos - 2) * PARTS + part if last else 2 * PARTS + part - 1
        sems = (rs_send.at[k, pos], rs_recv.at[k, pos]) if part == 0 and not last else (p_send.at[index], p_recv.at[index])
        return send(pbuf.at[k, pos, rows], dst, 'y' if pos % 2 else 'x', *sems)

    tile_spec = pl.BlockSpec((TILE, dim), lambda t: (t, 0), pipeline_mode=DEEP)
    out_spec = pl.BlockSpec((TILE, dim), lambda t: (t, 0), pipeline_mode=OUT)

    def scatter_last(k, h, far):
        wait_all(far)

        def body(p_ref, r_ref, s_ref):
            s_ref[...] = p_ref[...] + r_ref[...]
        pltpu.emit_pipeline(body, grid=(half // TILE,), in_specs=[tile_spec] * 2, out_specs=[out_spec])(
            pbuf.at[k, 4 + h], precv.at[k, h], sbuf.at[k, h])
        return send(sbuf.at[k, h], precv.at[k, 4 + h], 'x' if h else 'y', rs_send.at[k, 4 + h], rs_recv.at[k, 4 + h])

    def scatter_finish(k, h, near, last):
        near.wait_recv()
        last.wait_recv()

        def body(p_ref, n_ref, l_ref, u_ref):
            u_ref[...] = ((p_ref[...] + n_ref[...]) + l_ref[...]).astype(BF16)
        pltpu.emit_pipeline(body, grid=(half // TILE,), in_specs=[tile_spec] * 3, out_specs=[out_spec])(
            pbuf.at[k, 6 + h], precv.at[k, 2 + h], precv.at[k, 4 + h], upan.at[k + 1, 6 + h])

    def item_layer(k):
        copy = send(acc.at[1 - r], qrecv.at[k - 1], 'r', q_send.at[k - 1], q_recv.at[k - 1])
        copy.wait_recv()
        rows = jnp.transpose(acc[r] + qrecv[k - 1]).astype(BF16)
        vtot[...] += rows.astype(F32)
        finish(copy)
        if k < LAYERS:
            vpan[k, r] = rows
            other = send(vpan.at[k, r], vpan.at[k, r], 'r', v_send.at[k], v_recv.at[k])
            acc[...] = jnp.zeros_like(acc)
            other.wait_recv()

    vtot[...] = vpan[0, r].astype(F32)
    for j in range(3):
        row = jnp.broadcast_to(ids[j:j + 1, :].astype(F32), (LANES, batch))
        idcol[j] = jnp.transpose(row).astype(jnp.int32)
    far, near = {}, {}
    build(0, 1, None)
    far[0, 0] = [scatter_send(0, 0)]
    far[0, 1] = []
    for part in range(2):
        build(1, 1, None, part * (half // BUILD // 2), half // BUILD // 2)
        far[0, 1].append(scatter_send(0, 1, part, 2))
    build(2, 1, (upan.at[0], 0))
    near[0, 0] = scatter_send(0, 2)
    build(3, 1, (upan.at[0], 0))
    near[0, 1] = scatter_send(0, 3)
    wait_all(rest0[:2])
    build(4, 2, (upan.at[0], 0))
    build(6, 2, (user0, 6))
    wait_all(rest0[2:])
    last0 = [scatter_last(0, h, far[0, h]) for h in (0, 1)]
    accumulate(0, 2)
    item_layer(1)
    for pos in range(2):
        multiply(1, pos, 1)
        far[1, pos] = [scatter_send(1, pos)]
    multiply(1, 2, 6)
    for h in (0, 1):
        scatter_finish(0, h, near[0, h], last0[h])
    gather1 = gather_start(1)
    rest1 = gather_forward(1, gather1)
    for pos in (2, 3):
        near[1, pos % 2] = scatter_send(1, pos)
    last1 = [scatter_last(1, h, far[1, h]) for h in (0, 1)]
    wait_all(rest1)
    accumulate(1, 8)
    item_layer(2)
    for pos in range(2):
        multiply(2, pos, 1)
        far[2, pos] = [scatter_send(2, pos)]
    multiply(2, 2, 6)
    for h in (0, 1):
        scatter_finish(1, h, near[1, h], last1[h])
    gather2 = gather_start(2)
    rest2 = gather_forward(2, gather2)
    last2 = [scatter_last(2, h, far[2, h]) for h in (0, 1)]
    wait_all(rest2)
    accumulate(2, 8)
    item_layer(3)

    out_rows = (vtot[...] / (LAYERS + 1)).astype(BF16)
    item_out[...] = out_rows
    item_base = ((y * 2 + x) * 2 + r) * own_items
    for j in range(2):
        hit = (idcol[1 + j, :, 0:1] - item_base) == lax.broadcasted_iota(jnp.int32, (batch, own_items), 1)
        selb[j] = jnp.dot(hit.astype(BF16), out_rows, preferred_element_type=F32).astype(BF16)
    core = send(selb.at[1 - r], selrecv.at[0], 'r', e_send.at[0], e_recv.at[0])
    core.wait_recv()
    sel[0] = selb[r] + selrecv[0]
    xrow = send(sel.at[0], selrecv.at[1], 'x', e_send.at[1], e_recv.at[1])
    parts = {2: [scatter_send(2, 2, 0, PARTS)], 3: [scatter_send(2, 3, 0, PARTS)]}
    xrow.wait_recv()
    sel[1] = sel[0] + selrecv[1]
    yrow = send(sel.at[1], selrecv.at[2], 'y', e_send.at[2], e_recv.at[2])
    for part in range(1, PARTS):
        for pos in (2, 3):
            parts[pos].append(scatter_send(2, pos, part, PARTS))

    for h in (0, 1):
        last2[h].wait_recv()

        def body(p_ref, l_ref, u0_ref, u1_ref, u2_ref, h=h):
            rows = pl.ds(pl.multiple_of(pl.program_id(0) * TILE, TILE), TILE)
            base[h, rows, :] = p_ref[...] + l_ref[...]
            usum[h, rows, :] = (u0_ref[...].astype(F32) + u1_ref[...].astype(F32)) + u2_ref[...].astype(F32)
        pltpu.emit_pipeline(body, grid=(half // TILE,), in_specs=[tile_spec] * 5)(
            pbuf.at[2, 6 + h], precv.at[2, 4 + h], user0.at[h], upan.at[1, 6 + h], upan.at[2, 6 + h])
    yrow.wait_recv()
    finish(core)
    selb[r] = sel[1] + selrecv[2]
    back = send(selb.at[r], selrecv.at[3], 'r', e_send.at[3], e_recv.at[3])
    back.wait_recv()

    user_base = ((r * 2 + y) * 2 + x) * (2 * half)
    local = idcol[0, :, 0:1] - user_base
    mine[...] = jnp.zeros_like(mine)
    size = half // PARTS
    for part in range(PARTS):
        rows = pl.ds(part * size, size)
        for h in (0, 1):
            parts[2 + h][part].wait_recv()
            last_user = (base[h, rows, :] + nearv[h, rows, :]).astype(BF16)
            mean = ((usum[h, rows, :] + last_user.astype(F32)) / (LAYERS + 1)).astype(BF16)
            user_out[h, rows, :] = mean
            hit = (local - (h * half + part * size)) == lax.broadcasted_iota(jnp.int32, (batch, size), 1)
            mine[...] += jnp.dot(hit.astype(BF16), mean, preferred_element_type=F32)
    own_rows, other_rows = selb[r].astype(F32), selrecv[3].astype(F32)
    pos_rows = jnp.where(r == 0, own_rows, other_rows)
    neg_rows = jnp.where(r == 0, other_rows, own_rows)
    rows = mine[...]
    margin = (jnp.sum(rows * pos_rows, axis=1, keepdims=True) - jnp.sum(rows * neg_rows, axis=1, keepdims=True)) / math.sqrt(dim)
    soft = jnp.maximum(-margin, 0.0) + jnp.log1p(jnp.exp(-jnp.abs(margin)))
    terms = jnp.where((local >= 0) & (local < 2 * half), soft, 0.0)
    lsend[...] = jnp.broadcast_to(jnp.sum(terms, axis=0, keepdims=True), (8, LANES))
    shared = [send_to(lsend, lrecv.at[i], device, l_send.at[i], l_recv.at[i]) for i, device in enumerate(others)]
    for copy in pending:
        copy.wait_send()
    wait_all(shared)
    level = [lsend[...]] + [lrecv[i] for i in range(len(others))]
    while len(level) > 1:
        level = [level[i] + level[i + 1] for i in range(0, len(level), 2)]
    loss_out[...] = level[0][0:1, 0:1] / batch


def solution(mesh):
    def device_program(mask_blk, user_shard, item_shard, triples):
        shard, dim = user_shard.shape
        half, items, own_items, batch = shard // 2, mask_blk.shape[1], item_shard.shape[0], triples.shape[0]
        hbm = pl.BlockSpec(memory_space=pltpu.HBM)
        vmem = pl.BlockSpec(memory_space=pltpu.VMEM)
        shapes = [((2, half, dim), BF16), ((own_items, dim), BF16), ((1, 1), F32), ((8, half, items), BF16),
                  ((LAYERS, 8, half, dim), BF16), ((LAYERS, 8, half, dim), F32), ((LAYERS, 6, half, dim), F32),
                  ((LAYERS, 2, half, dim), F32)]
        dma = pltpu.SemaphoreType.DMA
        outs = pl.pallas_call(
            functools.partial(kernel, (half, items, own_items, dim)),
            out_shape=[jax.ShapeDtypeStruct(*shape) for shape in shapes],
            in_specs=[hbm] * 4,
            out_specs=[vmem, vmem, vmem] + [hbm] * 5,
            scratch_shapes=[
                pltpu.VMEM((LAYERS, 2, own_items, dim), BF16), pltpu.VMEM((2, dim, own_items), F32),
                pltpu.VMEM((LAYERS, dim, own_items), F32), pltpu.VMEM((own_items, dim), F32),
                pltpu.VMEM((8, 8, BUILD), F32), pltpu.VMEM((BUILD, LANES), F32), pltpu.VMEM((1, items), F32),
                pltpu.VMEM((8, 8, BUILD), F32), pltpu.VMEM((2, 8, 8, BUILD), F32),
                pltpu.VMEM((8, items), F32), pltpu.VMEM((8, items), F32),
                pltpu.VMEM((2, batch, dim), BF16), pltpu.VMEM((2, batch, dim), BF16), pltpu.VMEM((4, batch, dim), BF16),
                pltpu.VMEM((batch, dim), F32), pltpu.VMEM((8, LANES), F32), pltpu.VMEM((7, 8, LANES), F32),
                pltpu.VMEM((3, batch), jnp.int32), pltpu.VMEM((3, batch, LANES), jnp.int32),
                pltpu.VMEM((2, half, dim), F32), pltpu.VMEM((2, half, dim), F32), pltpu.VMEM((2, half, dim), F32),
                dma((2,)),
                dma((LAYERS, 6)), dma((LAYERS, 6)), dma((LAYERS, 6)), dma((LAYERS, 6)), dma((2 * PARTS + 1,)), dma((2 * PARTS + 1,)), dma((LAYERS,)), dma((LAYERS,)),
                dma((LAYERS,)), dma((LAYERS,)), dma((4,)), dma((4,)), dma((4,)), dma((4,)), dma((7,)), dma((7,))],
            compiler_params=pltpu.CompilerParams(collective_id=0, has_side_effects=True, vmem_limit_bytes=48 * 1024 * 1024),
        )(*[pltpu.with_memory_space_constraint(a, pltpu.HBM) for a in (mask_blk, user_shard.reshape(2, half, dim), item_shard, triples.T)])
        return outs[0].reshape(shard, dim), outs[1], outs[2].reshape(())

    return jax.shard_map(device_program, mesh=mesh, in_specs=(P('row', COL_AXES), P(USER_AXES, None), P(ITEM_AXES, None), P()), out_specs=(P(USER_AXES, None), P(ITEM_AXES, None), P()), check_vma=False)
```

```python
import functools
import itertools
import math
import jax
import jax.numpy as jnp
from jax import lax
from jax.experimental import pallas as pl
from jax.experimental.pallas import tpu as pltpu
from jax.sharding import PartitionSpec as P

LAYERS = 3
USER_AXES = ('row', 'cola', 'colb')
ITEM_AXES = ('cola', 'colb', 'row')
COL_AXES = ('cola', 'colb')
F32 = jnp.float32
BF16 = jnp.bfloat16
CONTRACT_ROWS = (((0,), (0,)), ((), ()))
CONTRACT_COLS = (((1,), (1,)), ((), ()))
BUILD = 256
TILE = 512
CHUNK = 32
PARTS = 4
HEAD = 320
DEEP = pl.Buffered(4)
OUT = pl.Buffered(2)
LANES = 128


def kernel(dims, mask, user0, item0, triples, user_out, item_out, loss_out, adj, upan, pbuf, precv, sbuf,
           vpan, acc, qrecv, vtot, us, uscol, isc, degu, drecv, degi, degi_recv, sel, selb, selrecv, mine, lsend, lrecv,
           ids, idcol, base, usum, nearv, local_sem,
           ag_send, ag_recv, rs_send, rs_recv, p_send, p_recv, v_send, v_recv, q_send, q_recv, d_send, d_recv, e_send, e_recv, l_send, l_recv):
    half, items, own_items, dim = dims
    x, y, r = lax.axis_index('colb'), lax.axis_index('cola'), lax.axis_index('row')
    to = {'x': {'colb': 1 - x}, 'y': {'cola': 1 - y}, 'r': {'row': 1 - r},
          'xy': {'colb': 1 - x, 'cola': 1 - y}}
    others = [{'cola': 1 - y if dy else y, 'colb': 1 - x if dx else x, 'row': 1 - r if dr else r}
              for dy, dx, dr in itertools.product((0, 1), repeat=3) if dy or dx or dr]
    pending = []
    batch = ids.shape[1]

    def send_to(src, dst, device, send_sem, recv_sem):
        copy = pltpu.make_async_remote_copy(src_ref=src, dst_ref=dst, send_sem=send_sem, recv_sem=recv_sem,
                                            device_id=device, device_id_type=pl.DeviceIdType.MESH)
        copy.start()
        pending.append(copy)
        return copy

    def send(src, dst, direction, send_sem, recv_sem):
        return send_to(src, dst, to[direction], send_sem, recv_sem)

    def finish(copy):
        copy.wait_send()
        pending[:] = [other for other in pending if other is not copy]

    item_in = pltpu.make_async_copy(item0, vpan.at[0, r], local_sem.at[0])
    ids_in = pltpu.make_async_copy(triples, ids, local_sem.at[1])
    item_in.start()
    ids_in.start()
    barrier = pltpu.get_barrier_semaphore()
    for device in others:
        pl.semaphore_signal(barrier, inc=1, device_id=device, device_id_type=pl.DeviceIdType.MESH)
    pl.semaphore_wait(barrier, len(others))

    def own(k, h):
        return user0.at[h] if k == 0 else upan.at[k, 6 + h]

    def gather_start(k):
        return [send(own(k, 0), upan.at[k, 2], 'x', ag_send.at[k, 0], ag_recv.at[k, 0]),
                send(own(k, 1), upan.at[k, 3], 'y', ag_send.at[k, 1], ag_recv.at[k, 1]),
                send(own(k, 0), upan.at[k, 4], 'y', ag_send.at[k, 2], ag_recv.at[k, 2]),
                send(own(k, 1), upan.at[k, 5], 'x', ag_send.at[k, 3], ag_recv.at[k, 3])]

    def gather_forward(k, copies):
        copies[0].wait_recv()
        far0 = send(upan.at[k, 2], upan.at[k, 0], 'y', ag_send.at[k, 4], ag_recv.at[k, 4])
        copies[1].wait_recv()
        far1 = send(upan.at[k, 3], upan.at[k, 1], 'x', ag_send.at[k, 5], ag_recv.at[k, 5])
        return copies[2:] + [far0, far1]

    def wait_all(copies):
        for copy in copies:
            copy.wait_recv()

    gather0 = gather_start(0)
    item_in.wait()
    ids_in.wait()
    item_copy = send(item0, vpan.at[0, r], 'r', v_send.at[0], v_recv.at[0])

    def mask_block(pos, tile):
        h, q = lax.rem(pos, 2), lax.div(pos, 2)
        prim, sec = 1 - lax.div(q, 2), 1 - lax.rem(q, 2)
        dx, dy = prim * (1 - h) + sec * h, sec * (1 - h) + prim * h
        shard = lax.rem(y + dy, 2) * 2 + lax.rem(x + dx, 2)
        return (shard * 2 + h) * (half // BUILD) + tile

    degu[...] = jnp.zeros_like(degu)
    degi[...] = jnp.zeros_like(degi)
    acc[...] = jnp.zeros_like(acc)

    def degree_body(m_ref):
        pos, tile = pl.program_id(0), pl.program_id(1)

        def chunk(i, cols):
            m = m_ref[pl.ds(pl.multiple_of(i * CHUNK, CHUNK), CHUNK), :]
            part = m[:, :LANES]
            for j in range(1, items // LANES):
                part = part + m[:, j * LANES:(j + 1) * LANES]
            uscol[pl.ds(pl.multiple_of(i * CHUNK, CHUNK), CHUNK), :] = part.astype(F32)
            for j in range(CHUNK // 8):
                cols = cols + m[j * 8:(j + 1) * 8, :]
            return cols

        cols = lax.fori_loop(0, BUILD // CHUNK, chunk, jnp.zeros((8, items), jnp.int32))
        degi[...] += cols.astype(F32)
        pick = (lax.broadcasted_iota(jnp.int32, (8, LANES), 0) == tile).astype(BF16)
        degu[pos] += lax.dot_general(pick, uscol[...].astype(BF16), CONTRACT_COLS, preferred_element_type=F32)

    pltpu.emit_pipeline(degree_body, grid=(8, half // BUILD),
                        in_specs=[pl.BlockSpec((BUILD, items), lambda p, t: (mask_block(p, t), 0), pipeline_mode=DEEP)])(mask)
    item_deg = send(degi, degi_recv, 'r', d_send.at[0], d_recv.at[0])
    user_deg = send(degu, drecv.at[0], 'x', d_send.at[1], d_recv.at[1])
    head, tail = pl.ds(0, HEAD), pl.ds(HEAD, half - HEAD)
    gather0[0].wait_recv()
    rest0 = gather0[2:] + [send(upan.at[0, 2, head], upan.at[0, 0, head], 'y', ag_send.at[0, 4], ag_recv.at[0, 4])]
    gather0[1].wait_recv()
    rest0.append(send(upan.at[0, 3], upan.at[0, 1], 'x', ag_send.at[0, 5], ag_recv.at[0, 5]))
    user_deg.wait_recv()
    for pos in range(8):
        us[pos] = degu[pos] + drecv[0, pos ^ (2 if pos % 2 else 4)]
    user_deg2 = send(us, drecv.at[1], 'y', d_send.at[2], d_recv.at[2])
    rest0.append(send(upan.at[0, 2, tail], upan.at[0, 0, tail], 'y', d_send.at[3], d_recv.at[3]))
    item_deg.wait_recv()
    total = jnp.sum(degi[...] + degi_recv[...], axis=0, keepdims=True)
    isc[...] = lax.rsqrt(jnp.maximum(total, 1.0))
    user_deg2.wait_recv()
    finish(user_deg)
    for pos in range(8):
        degu[pos] = lax.rsqrt(jnp.maximum(us[pos] + drecv[1, pos ^ (4 if pos % 2 else 2)], 1.0))
    item_copy.wait_recv()

    def panel(k):
        return vpan[k].reshape(items, dim)

    def add_items(a_ref, u_ref):
        for j in range(2):
            acc[j] += lax.dot_general(u_ref[...], a_ref[:, j * own_items:(j + 1) * own_items], CONTRACT_ROWS,
                                      preferred_element_type=F32)

    def build(first, count, users, start_tile=0, tiles=half // BUILD):
        def body(m_ref, *refs):
            (u_ref, a_ref, p_ref) = refs if users is not None else (None,) + refs
            pos, tile = pl.program_id(0) + first, pl.program_id(1) + start_tile
            row = degu[pos, pl.ds(tile, 1), :]
            uscol[...] = jnp.transpose(jnp.broadcast_to(row, (LANES, BUILD)))

            def chunk(i, carry):
                rows = pl.ds(pl.multiple_of(i * CHUNK, CHUNK), CHUNK)
                scale = uscol[rows, :]
                for j in range(items // LANES):
                    cols = slice(j * LANES, (j + 1) * LANES)
                    weight = (scale * m_ref[rows, cols].astype(F32)) * isc[:, cols]
                    a_ref[rows, cols] = weight.astype(BF16)
                return carry

            lax.fori_loop(0, BUILD // CHUNK, chunk, 0)
            p_ref[...] = jnp.dot(a_ref[...], panel(0), preferred_element_type=F32)
            if users is not None:
                add_items(a_ref, u_ref)

        operands = [mask]
        in_specs = [pl.BlockSpec((BUILD, items), lambda p, t: (mask_block(p + first, t + start_tile), 0), pipeline_mode=DEEP)]
        if users is not None:
            ref, start = users
            operands.append(ref)
            in_specs.append(pl.BlockSpec((None, BUILD, dim), lambda p, t: (p + (first - start), t + start_tile, 0), pipeline_mode=DEEP))
        pltpu.emit_pipeline(body, grid=(count, tiles), in_specs=in_specs,
                            out_specs=[pl.BlockSpec((None, BUILD, items), lambda p, t: (p + first, t + start_tile, 0), pipeline_mode=OUT),
                                       pl.BlockSpec((None, BUILD, dim), lambda p, t: (p + first, t + start_tile, 0), pipeline_mode=OUT)])(*operands, adj, pbuf.at[0])

    def multiply(k, first, count):
        def body(a_ref, p_ref):
            p_ref[...] = jnp.dot(a_ref[...], panel(k), preferred_element_type=F32)
        pltpu.emit_pipeline(body, grid=(count, half // TILE),
                            in_specs=[pl.BlockSpec((None, TILE, items), lambda p, t: (p + first, t, 0), pipeline_mode=DEEP)],
                            out_specs=[pl.BlockSpec((None, TILE, dim), lambda p, t: (p + first, t, 0), pipeline_mode=OUT)])(adj, pbuf.at[k])

    def accumulate(k, count):
        pltpu.emit_pipeline(add_items, grid=(count, half // TILE),
                            in_specs=[pl.BlockSpec((None, TILE, items), lambda p, t: (p, t, 0), pipeline_mode=DEEP),
                                      pl.BlockSpec((None, TILE, dim), lambda p, t: (p, t, 0), pipeline_mode=DEEP)])(adj, upan.at[k])

    def scatter_send(k, pos, part=0, parts=1):
        rows = pl.ds(part * (half // parts), half // parts)
        last = k == LAYERS - 1 and pos >= 2
        dst = nearv.at[pos - 2, rows] if last else precv.at[k, pos, rows]
        index = (pos - 2) * PARTS + part if last else 2 * PARTS + part - 1
        sems = (rs_send.at[k, pos], rs_recv.at[k, pos]) if part == 0 and not last else (p_send.at[index], p_recv.at[index])
        return send(pbuf.at[k, pos, rows], dst, 'y' if pos % 2 else 'x', *sems)

    tile_spec = pl.BlockSpec((TILE, dim), lambda t: (t, 0), pipeline_mode=DEEP)
    out_spec = pl.BlockSpec((TILE, dim), lambda t: (t, 0), pipeline_mode=OUT)

    def scatter_last(k, h, far):
        wait_all(far)

        def body(p_ref, r_ref, s_ref):
            s_ref[...] = p_ref[...] + r_ref[...]
        pltpu.emit_pipeline(body, grid=(half // TILE,), in_specs=[tile_spec] * 2, out_specs=[out_spec])(
            pbuf.at[k, 4 + h], precv.at[k, h], sbuf.at[k, h])
        return send(sbuf.at[k, h], precv.at[k, 4 + h], 'x' if h else 'y', rs_send.at[k, 4 + h], rs_recv.at[k, 4 + h])

    def scatter_finish(k, h, near, last):
        near.wait_recv()
        last.wait_recv()

        def body(p_ref, n_ref, l_ref, u_ref):
            u_ref[...] = ((p_ref[...] + n_ref[...]) + l_ref[...]).astype(BF16)
        pltpu.emit_pipeline(body, grid=(half // TILE,), in_specs=[tile_spec] * 3, out_specs=[out_spec])(
            pbuf.at[k, 6 + h], precv.at[k, 2 + h], precv.at[k, 4 + h], upan.at[k + 1, 6 + h])

    def item_layer(k):
        copy = send(acc.at[1 - r], qrecv.at[k - 1], 'r', q_send.at[k - 1], q_recv.at[k - 1])
        copy.wait_recv()
        rows = jnp.transpose(acc[r] + qrecv[k - 1]).astype(BF16)
        vtot[...] += rows.astype(F32)
        finish(copy)
        if k < LAYERS:
            vpan[k, r] = rows
            other = send(vpan.at[k, r], vpan.at[k, r], 'r', v_send.at[k], v_recv.at[k])
            acc[...] = jnp.zeros_like(acc)
            other.wait_recv()

    vtot[...] = vpan[0, r].astype(F32)
    for j in range(3):
        row = jnp.broadcast_to(ids[j:j + 1, :].astype(F32), (LANES, batch))
        idcol[j] = jnp.transpose(row).astype(jnp.int32)
    far, near = {}, {}
    build(0, 1, None)
    far[0, 0] = [scatter_send(0, 0)]
    far[0, 1] = []
    for part in range(2):
        build(1, 1, None, part * (half // BUILD // 2), half // BUILD // 2)
        far[0, 1].append(scatter_send(0, 1, part, 2))
    build(2, 1, (upan.at[0], 0))
    near[0, 0] = scatter_send(0, 2)
    build(3, 1, (upan.at[0], 0))
    near[0, 1] = scatter_send(0, 3)
    wait_all(rest0[:2])
    build(4, 2, (upan.at[0], 0))
    build(6, 2, (user0, 6))
    wait_all(rest0[2:])
    last0 = [scatter_last(0, h, far[0, h]) for h in (0, 1)]
    accumulate(0, 2)
    item_layer(1)
    for pos in range(2):
        multiply(1, pos, 1)
        far[1, pos] = [scatter_send(1, pos)]
    multiply(1, 2, 6)
    for h in (0, 1):
        scatter_finish(0, h, near[0, h], last0[h])
    gather1 = gather_start(1)
    rest1 = gather_forward(1, gather1)
    for pos in (2, 3):
        near[1, pos % 2] = scatter_send(1, pos)
    last1 = [scatter_last(1, h, far[1, h]) for h in (0, 1)]
    wait_all(rest1)
    accumulate(1, 8)
    item_layer(2)
    for pos in range(2):
        multiply(2, pos, 1)
        far[2, pos] = [scatter_send(2, pos)]
    multiply(2, 2, 6)
    for h in (0, 1):
        scatter_finish(1, h, near[1, h], last1[h])
    gather2 = gather_start(2)
    rest2 = gather_forward(2, gather2)
    last2 = [scatter_last(2, h, far[2, h]) for h in (0, 1)]
    wait_all(rest2)
    accumulate(2, 8)
    item_layer(3)

    out_rows = (vtot[...] / (LAYERS + 1)).astype(BF16)
    item_out[...] = out_rows
    item_base = ((y * 2 + x) * 2 + r) * own_items
    for j in range(2):
        hit = (idcol[1 + j, :, 0:1] - item_base) == lax.broadcasted_iota(jnp.int32, (batch, own_items), 1)
        selb[j] = jnp.dot(hit.astype(BF16), out_rows, preferred_element_type=F32).astype(BF16)
    core = send(selb.at[1 - r], selrecv.at[0], 'r', e_send.at[0], e_recv.at[0])
    core.wait_recv()
    sel[0] = selb[r] + selrecv[0]
    xrow = send(sel.at[0], selrecv.at[1], 'x', e_send.at[1], e_recv.at[1])
    parts = {2: [scatter_send(2, 2, 0, PARTS)], 3: [scatter_send(2, 3, 0, PARTS)]}
    xrow.wait_recv()
    sel[1] = sel[0] + selrecv[1]
    yrow = send(sel.at[1], selrecv.at[2], 'y', e_send.at[2], e_recv.at[2])
    for part in range(1, PARTS):
        for pos in (2, 3):
            parts[pos].append(scatter_send(2, pos, part, PARTS))

    for h in (0, 1):
        last2[h].wait_recv()

        def body(p_ref, l_ref, u0_ref, u1_ref, u2_ref, h=h):
            rows = pl.ds(pl.multiple_of(pl.program_id(0) * TILE, TILE), TILE)
            base[h, rows, :] = p_ref[...] + l_ref[...]
            usum[h, rows, :] = (u0_ref[...].astype(F32) + u1_ref[...].astype(F32)) + u2_ref[...].astype(F32)
        pltpu.emit_pipeline(body, grid=(half // TILE,), in_specs=[tile_spec] * 5)(
            pbuf.at[2, 6 + h], precv.at[2, 4 + h], user0.at[h], upan.at[1, 6 + h], upan.at[2, 6 + h])
    yrow.wait_recv()
    finish(core)
    selb[r] = sel[1] + selrecv[2]
    back = send(selb.at[r], selrecv.at[3], 'r', e_send.at[3], e_recv.at[3])
    back.wait_recv()

    user_base = ((r * 2 + y) * 2 + x) * (2 * half)
    local = idcol[0, :, 0:1] - user_base
    mine[...] = jnp.zeros_like(mine)
    size = half // PARTS
    for part in range(PARTS):
        rows = pl.ds(part * size, size)
        for h in (0, 1):
            parts[2 + h][part].wait_recv()
            last_user = (base[h, rows, :] + nearv[h, rows, :]).astype(BF16)
            mean = ((usum[h, rows, :] + last_user.astype(F32)) / (LAYERS + 1)).astype(BF16)
            user_out[h, rows, :] = mean
            hit = (local - (h * half + part * size)) == lax.broadcasted_iota(jnp.int32, (batch, size), 1)
            mine[...] += jnp.dot(hit.astype(BF16), mean, preferred_element_type=F32)
    own_rows, other_rows = selb[r].astype(F32), selrecv[3].astype(F32)
    pos_rows = jnp.where(r == 0, own_rows, other_rows)
    neg_rows = jnp.where(r == 0, other_rows, own_rows)
    rows = mine[...]
    margin = (jnp.sum(rows * pos_rows, axis=1, keepdims=True) - jnp.sum(rows * neg_rows, axis=1, keepdims=True)) / math.sqrt(dim)
    soft = jnp.maximum(-margin, 0.0) + jnp.log1p(jnp.exp(-jnp.abs(margin)))
    terms = jnp.where((local >= 0) & (local < 2 * half), soft, 0.0)
    lsend[...] = jnp.broadcast_to(jnp.sum(terms, axis=0, keepdims=True), (8, LANES))
    shared = [send_to(lsend, lrecv.at[i], device, l_send.at[i], l_recv.at[i]) for i, device in enumerate(others)]
    for copy in pending:
        copy.wait_send()
    wait_all(shared)
    level = [lsend[...]] + [lrecv[i] for i in range(len(others))]
    while len(level) > 1:
        level = [level[i] + level[i + 1] for i in range(0, len(level), 2)]
    loss_out[...] = level[0][0:1, 0:1] / batch


def solution(mesh):
    def device_program(mask_blk, user_shard, item_shard, triples):
        shard, dim = user_shard.shape
        half, items, own_items, batch = shard // 2, mask_blk.shape[1], item_shard.shape[0], triples.shape[0]
        hbm = pl.BlockSpec(memory_space=pltpu.HBM)
        vmem = pl.BlockSpec(memory_space=pltpu.VMEM)
        shapes = [((2, half, dim), BF16), ((own_items, dim), BF16), ((1, 1), F32), ((8, half, items), BF16),
                  ((LAYERS, 8, half, dim), BF16), ((LAYERS, 8, half, dim), F32), ((LAYERS, 6, half, dim), F32),
                  ((LAYERS, 2, half, dim), F32)]
        dma = pltpu.SemaphoreType.DMA
        outs = pl.pallas_call(
            functools.partial(kernel, (half, items, own_items, dim)),
            out_shape=[jax.ShapeDtypeStruct(*shape) for shape in shapes],
            in_specs=[hbm] * 4,
            out_specs=[vmem, vmem, vmem] + [hbm] * 5,
            scratch_shapes=[
                pltpu.VMEM((LAYERS, 2, own_items, dim), BF16), pltpu.VMEM((2, dim, own_items), F32),
                pltpu.VMEM((LAYERS, dim, own_items), F32), pltpu.VMEM((own_items, dim), F32),
                pltpu.VMEM((8, 8, BUILD), F32), pltpu.VMEM((BUILD, LANES), F32), pltpu.VMEM((1, items), F32),
                pltpu.VMEM((8, 8, BUILD), F32), pltpu.VMEM((2, 8, 8, BUILD), F32),
                pltpu.VMEM((8, items), F32), pltpu.VMEM((8, items), F32),
                pltpu.VMEM((2, batch, dim), BF16), pltpu.VMEM((2, batch, dim), BF16), pltpu.VMEM((4, batch, dim), BF16),
                pltpu.VMEM((batch, dim), F32), pltpu.VMEM((8, LANES), F32), pltpu.VMEM((7, 8, LANES), F32),
                pltpu.VMEM((3, batch), jnp.int32), pltpu.VMEM((3, batch, LANES), jnp.int32),
                pltpu.VMEM((2, half, dim), F32), pltpu.VMEM((2, half, dim), F32), pltpu.VMEM((2, half, dim), F32),
                dma((2,)),
                dma((LAYERS, 6)), dma((LAYERS, 6)), dma((LAYERS, 6)), dma((LAYERS, 6)), dma((2 * PARTS + 1,)), dma((2 * PARTS + 1,)), dma((LAYERS,)), dma((LAYERS,)),
                dma((LAYERS,)), dma((LAYERS,)), dma((4,)), dma((4,)), dma((4,)), dma((4,)), dma((7,)), dma((7,))],
            compiler_params=pltpu.CompilerParams(collective_id=0, has_side_effects=True, vmem_limit_bytes=48 * 1024 * 1024),
        )(*[pltpu.with_memory_space_constraint(a, pltpu.HBM) for a in (mask_blk, user_shard.reshape(2, half, dim), item_shard, triples.T)])
        return outs[0].reshape(shard, dim), outs[1], outs[2].reshape(())

    return jax.shard_map(device_program, mesh=mesh, in_specs=(P('row', COL_AXES), P(USER_AXES, None), P(ITEM_AXES, None), P()), out_specs=(P(USER_AXES, None), P(ITEM_AXES, None), P()), check_vma=False)
```

```python
import functools
import itertools
import math
import jax
import jax.numpy as jnp
from jax import lax
from jax.experimental import pallas as pl
from jax.experimental.pallas import tpu as pltpu
from jax.sharding import PartitionSpec as P

LAYERS = 3
USER_AXES = ('row', 'cola', 'colb')
ITEM_AXES = ('cola', 'colb', 'row')
COL_AXES = ('cola', 'colb')
F32 = jnp.float32
BF16 = jnp.bfloat16
CONTRACT_ROWS = (((0,), (0,)), ((), ()))
CONTRACT_COLS = (((1,), (1,)), ((), ()))
BUILD = 256
TILE = 512
CHUNK = 32
PARTS = 4
HEAD = 320
DEEP = pl.Buffered(4)
OUT = pl.Buffered(2)
LANES = 128


def kernel(dims, mask, user0, item0, triples, user_out, item_out, loss_out, adj, upan, pbuf, precv, sbuf,
           vpan, acc, qrecv, vtot, us, uscol, isc, degu, drecv, degi, degi_recv, sel, selb, selrecv, mine, lsend, lrecv,
           ids, idcol, base, usum, nearv, local_sem,
           ag_send, ag_recv, rs_send, rs_recv, p_recv, v_send, v_recv, q_send, q_recv, d_send, d_recv, e_send, e_recv, l_send, l_recv):
    half, items, own_items, dim = dims
    x, y, r = lax.axis_index('colb'), lax.axis_index('cola'), lax.axis_index('row')
    to = {'x': {'colb': 1 - x}, 'y': {'cola': 1 - y}, 'r': {'row': 1 - r},
          'xy': {'colb': 1 - x, 'cola': 1 - y}}
    others = [{'cola': 1 - y if dy else y, 'colb': 1 - x if dx else x, 'row': 1 - r if dr else r}
              for dy, dx, dr in itertools.product((0, 1), repeat=3) if dy or dx or dr]
    pending = []
    batch = ids.shape[1]

    def send_to(src, dst, device, send_sem, recv_sem, shared=False):
        copy = pltpu.make_async_remote_copy(src_ref=src, dst_ref=dst, send_sem=send_sem, recv_sem=recv_sem,
                                            device_id=device, device_id_type=pl.DeviceIdType.MESH)
        copy.start()
        if not shared:
            pending.append(copy)
        return copy

    def send(src, dst, direction, send_sem, recv_sem, shared=False):
        return send_to(src, dst, to[direction], send_sem, recv_sem, shared)

    def wait_sent(ref, send_sem, recv_sem):
        pltpu.make_async_remote_copy(src_ref=ref, dst_ref=ref, send_sem=send_sem, recv_sem=recv_sem,
                                     device_id=to['x'], device_id_type=pl.DeviceIdType.MESH).wait_send()

    def finish(copy):
        copy.wait_send()
        pending[:] = [other for other in pending if other is not copy]

    item_in = pltpu.make_async_copy(item0, vpan.at[0, r], local_sem.at[0])
    ids_in = pltpu.make_async_copy(triples, ids, local_sem.at[1])
    item_in.start()
    ids_in.start()
    barrier = pltpu.get_barrier_semaphore()
    for device in others:
        pl.semaphore_signal(barrier, inc=1, device_id=device, device_id_type=pl.DeviceIdType.MESH)
    pl.semaphore_wait(barrier, len(others))

    def own(k, h):
        return user0.at[h] if k == 0 else upan.at[k, 6 + h]

    def gather_start(k):
        return [send(own(k, 0), upan.at[k, 2], 'x', ag_send.at[k], ag_recv.at[k, 0], True),
                send(own(k, 1), upan.at[k, 3], 'y', ag_send.at[k], ag_recv.at[k, 1], True),
                send(own(k, 0), upan.at[k, 4], 'y', ag_send.at[k], ag_recv.at[k, 2], True),
                send(own(k, 1), upan.at[k, 5], 'x', ag_send.at[k], ag_recv.at[k, 3], True)]

    def gather_forward(k, copies):
        copies[0].wait_recv()
        far0 = send(upan.at[k, 2], upan.at[k, 0], 'y', ag_send.at[k], ag_recv.at[k, 4], True)
        copies[1].wait_recv()
        far1 = send(upan.at[k, 3], upan.at[k, 1], 'x', ag_send.at[k], ag_recv.at[k, 5], True)
        return copies[2:] + [far0, far1]

    def wait_all(copies):
        for copy in copies:
            copy.wait_recv()

    gather0 = gather_start(0)
    item_in.wait()
    ids_in.wait()
    item_copy = send(item0, vpan.at[0, r], 'r', v_send.at[0], v_recv.at[0])

    def mask_block(pos, tile):
        h, q = lax.rem(pos, 2), lax.div(pos, 2)
        prim, sec = 1 - lax.div(q, 2), 1 - lax.rem(q, 2)
        dx, dy = prim * (1 - h) + sec * h, sec * (1 - h) + prim * h
        shard = lax.rem(y + dy, 2) * 2 + lax.rem(x + dx, 2)
        return (shard * 2 + h) * (half // BUILD) + tile

    degu[...] = jnp.zeros_like(degu)
    degi[...] = jnp.zeros_like(degi)
    acc[...] = jnp.zeros_like(acc)

    def degree_body(m_ref):
        pos, tile = pl.program_id(0), pl.program_id(1)

        def chunk(i, cols):
            m = m_ref[pl.ds(pl.multiple_of(i * CHUNK, CHUNK), CHUNK), :]
            part = m[:, :LANES]
            for j in range(1, items // LANES):
                part = part + m[:, j * LANES:(j + 1) * LANES]
            uscol[pl.ds(pl.multiple_of(i * CHUNK, CHUNK), CHUNK), :] = part.astype(F32)
            for j in range(CHUNK // 8):
                cols = cols + m[j * 8:(j + 1) * 8, :]
            return cols

        cols = lax.fori_loop(0, BUILD // CHUNK, chunk, jnp.zeros((8, items), jnp.int32))
        degi[...] += cols.astype(F32)
        pick = (lax.broadcasted_iota(jnp.int32, (8, LANES), 0) == tile).astype(BF16)
        degu[pos] += lax.dot_general(pick, uscol[...].astype(BF16), CONTRACT_COLS, preferred_element_type=F32)

    pltpu.emit_pipeline(degree_body, grid=(8, half // BUILD),
                        in_specs=[pl.BlockSpec((BUILD, items), lambda p, t: (mask_block(p, t), 0), pipeline_mode=DEEP)])(mask)
    item_deg = send(degi, degi_recv, 'r', d_send.at[0], d_recv.at[0])
    user_deg = send(degu, drecv.at[0], 'x', d_send.at[1], d_recv.at[1])
    head, tail = pl.ds(0, HEAD), pl.ds(HEAD, half - HEAD)
    gather0[0].wait_recv()
    rest0 = gather0[2:] + [send(upan.at[0, 2, head], upan.at[0, 0, head], 'y', ag_send.at[0], ag_recv.at[0, 4], True)]
    gather0[1].wait_recv()
    rest0.append(send(upan.at[0, 3], upan.at[0, 1], 'x', ag_send.at[0], ag_recv.at[0, 5], True))
    user_deg.wait_recv()
    for pos in range(8):
        us[pos] = degu[pos] + drecv[0, pos ^ (2 if pos % 2 else 4)]
    user_deg2 = send(us, drecv.at[1], 'y', d_send.at[2], d_recv.at[2])
    rest0.append(send(upan.at[0, 2, tail], upan.at[0, 0, tail], 'y', ag_send.at[0], d_recv.at[3], True))
    item_deg.wait_recv()
    total = jnp.sum(degi[...] + degi_recv[...], axis=0, keepdims=True)
    isc[...] = lax.rsqrt(jnp.maximum(total, 1.0))
    user_deg2.wait_recv()
    finish(user_deg)
    for pos in range(8):
        degu[pos] = lax.rsqrt(jnp.maximum(us[pos] + drecv[1, pos ^ (4 if pos % 2 else 2)], 1.0))
    item_copy.wait_recv()

    def panel(k):
        return vpan[k].reshape(items, dim)

    def add_items(a_ref, u_ref):
        for j in range(2):
            acc[j] += lax.dot_general(u_ref[...], a_ref[:, j * own_items:(j + 1) * own_items], CONTRACT_ROWS,
                                      preferred_element_type=F32)

    def build(first, count, users, start_tile=0, tiles=half // BUILD):
        def body(m_ref, *refs):
            (u_ref, a_ref, p_ref) = refs if users is not None else (None,) + refs
            pos, tile = pl.program_id(0) + first, pl.program_id(1) + start_tile
            row = degu[pos, pl.ds(tile, 1), :]
            uscol[...] = jnp.transpose(jnp.broadcast_to(row, (LANES, BUILD)))

            def chunk(i, carry):
                rows = pl.ds(pl.multiple_of(i * CHUNK, CHUNK), CHUNK)
                scale = uscol[rows, :]
                for j in range(items // LANES):
                    cols = slice(j * LANES, (j + 1) * LANES)
                    weight = (scale * m_ref[rows, cols].astype(F32)) * isc[:, cols]
                    a_ref[rows, cols] = weight.astype(BF16)
                return carry

            lax.fori_loop(0, BUILD // CHUNK, chunk, 0)
            p_ref[...] = jnp.dot(a_ref[...], panel(0), preferred_element_type=F32)
            if users is not None:
                add_items(a_ref, u_ref)

        operands = [mask]
        in_specs = [pl.BlockSpec((BUILD, items), lambda p, t: (mask_block(p + first, t + start_tile), 0), pipeline_mode=DEEP)]
        if users is not None:
            ref, start = users
            operands.append(ref)
            in_specs.append(pl.BlockSpec((None, BUILD, dim), lambda p, t: (p + (first - start), t + start_tile, 0), pipeline_mode=DEEP))
        pltpu.emit_pipeline(body, grid=(count, tiles), in_specs=in_specs,
                            out_specs=[pl.BlockSpec((None, BUILD, items), lambda p, t: (p + first, t + start_tile, 0), pipeline_mode=OUT),
                                       pl.BlockSpec((None, BUILD, dim), lambda p, t: (p + first, t + start_tile, 0), pipeline_mode=OUT)])(*operands, adj, pbuf.at[0])

    def multiply(k, first, count):
        def body(a_ref, p_ref):
            p_ref[...] = jnp.dot(a_ref[...], panel(k), preferred_element_type=F32)
        pltpu.emit_pipeline(body, grid=(count, half // TILE),
                            in_specs=[pl.BlockSpec((None, TILE, items), lambda p, t: (p + first, t, 0), pipeline_mode=DEEP)],
                            out_specs=[pl.BlockSpec((None, TILE, dim), lambda p, t: (p + first, t, 0), pipeline_mode=OUT)])(adj, pbuf.at[k])

    def accumulate(k, count):
        pltpu.emit_pipeline(add_items, grid=(count, half // TILE),
                            in_specs=[pl.BlockSpec((None, TILE, items), lambda p, t: (p, t, 0), pipeline_mode=DEEP),
                                      pl.BlockSpec((None, TILE, dim), lambda p, t: (p, t, 0), pipeline_mode=DEEP)])(adj, upan.at[k])

    def scatter_send(k, pos, part=0, parts=1):
        rows = pl.ds(part * (half // parts), half // parts)
        last = k == LAYERS - 1 and pos >= 2
        dst = nearv.at[pos - 2, rows] if last else precv.at[k, pos, rows]
        index = (pos - 2) * PARTS + part if last else 2 * PARTS + part - 1
        recv_sem = rs_recv.at[k, pos] if part == 0 and not last else p_recv.at[index]
        return send(pbuf.at[k, pos, rows], dst, 'y' if pos % 2 else 'x', rs_send.at[k], recv_sem, True)

    tile_spec = pl.BlockSpec((TILE, dim), lambda t: (t, 0), pipeline_mode=DEEP)
    out_spec = pl.BlockSpec((TILE, dim), lambda t: (t, 0), pipeline_mode=OUT)

    def scatter_last(k, h, far):
        wait_all(far)

        def body(p_ref, r_ref, s_ref):
            s_ref[...] = p_ref[...] + r_ref[...]
        pltpu.emit_pipeline(body, grid=(half // TILE,), in_specs=[tile_spec] * 2, out_specs=[out_spec])(
            pbuf.at[k, 4 + h], precv.at[k, h], sbuf.at[k, h])
        return send(sbuf.at[k, h], precv.at[k, 4 + h], 'x' if h else 'y', rs_send.at[k], rs_recv.at[k, 4 + h], True)

    def scatter_finish(k, h, near, last):
        near.wait_recv()
        last.wait_recv()

        def body(p_ref, n_ref, l_ref, u_ref):
            u_ref[...] = ((p_ref[...] + n_ref[...]) + l_ref[...]).astype(BF16)
        pltpu.emit_pipeline(body, grid=(half // TILE,), in_specs=[tile_spec] * 3, out_specs=[out_spec])(
            pbuf.at[k, 6 + h], precv.at[k, 2 + h], precv.at[k, 4 + h], upan.at[k + 1, 6 + h])

    def item_layer(k):
        copy = send(acc.at[1 - r], qrecv.at[k - 1], 'r', q_send.at[k - 1], q_recv.at[k - 1])
        copy.wait_recv()
        rows = jnp.transpose(acc[r] + qrecv[k - 1]).astype(BF16)
        vtot[...] += rows.astype(F32)
        finish(copy)
        if k < LAYERS:
            vpan[k, r] = rows
            other = send(vpan.at[k, r], vpan.at[k, r], 'r', v_send.at[k], v_recv.at[k])
            acc[...] = jnp.zeros_like(acc)
            other.wait_recv()

    vtot[...] = vpan[0, r].astype(F32)
    for j in range(3):
        row = jnp.broadcast_to(ids[j:j + 1, :].astype(F32), (LANES, batch))
        idcol[j] = jnp.transpose(row).astype(jnp.int32)
    far, near = {}, {}
    build(0, 1, None)
    far[0, 0] = [scatter_send(0, 0)]
    far[0, 1] = []
    for part in range(2):
        build(1, 1, None, part * (half // BUILD // 2), half // BUILD // 2)
        far[0, 1].append(scatter_send(0, 1, part, 2))
    build(2, 1, (upan.at[0], 0))
    near[0, 0] = scatter_send(0, 2)
    build(3, 1, (upan.at[0], 0))
    near[0, 1] = scatter_send(0, 3)
    wait_all(rest0[:2])
    build(4, 2, (upan.at[0], 0))
    build(6, 2, (user0, 6))
    wait_all(rest0[2:])
    last0 = [scatter_last(0, h, far[0, h]) for h in (0, 1)]
    accumulate(0, 2)
    item_layer(1)
    for pos in range(2):
        multiply(1, pos, 1)
        far[1, pos] = [scatter_send(1, pos)]
    multiply(1, 2, 6)
    for h in (0, 1):
        scatter_finish(0, h, near[0, h], last0[h])
    gather1 = gather_start(1)
    rest1 = gather_forward(1, gather1)
    for pos in (2, 3):
        near[1, pos % 2] = scatter_send(1, pos)
    last1 = [scatter_last(1, h, far[1, h]) for h in (0, 1)]
    wait_all(rest1)
    accumulate(1, 8)
    item_layer(2)
    for pos in range(2):
        multiply(2, pos, 1)
        far[2, pos] = [scatter_send(2, pos)]
    multiply(2, 2, 6)
    for h in (0, 1):
        scatter_finish(1, h, near[1, h], last1[h])
    gather2 = gather_start(2)
    rest2 = gather_forward(2, gather2)
    last2 = [scatter_last(2, h, far[2, h]) for h in (0, 1)]
    wait_all(rest2)
    accumulate(2, 8)
    item_layer(3)

    out_rows = (vtot[...] / (LAYERS + 1)).astype(BF16)
    item_out[...] = out_rows
    item_base = ((y * 2 + x) * 2 + r) * own_items
    for j in range(2):
        hit = (idcol[1 + j, :, 0:1] - item_base) == lax.broadcasted_iota(jnp.int32, (batch, own_items), 1)
        selb[j] = jnp.dot(hit.astype(BF16), out_rows, preferred_element_type=F32).astype(BF16)
    core = send(selb.at[1 - r], selrecv.at[0], 'r', e_send.at[0], e_recv.at[0])
    core.wait_recv()
    sel[0] = selb[r] + selrecv[0]
    xrow = send(sel.at[0], selrecv.at[1], 'x', e_send.at[1], e_recv.at[1])
    parts = {2: [scatter_send(2, 2, 0, PARTS)], 3: [scatter_send(2, 3, 0, PARTS)]}
    xrow.wait_recv()
    sel[1] = sel[0] + selrecv[1]
    yrow = send(sel.at[1], selrecv.at[2], 'y', e_send.at[2], e_recv.at[2])
    for part in range(1, PARTS):
        for pos in (2, 3):
            parts[pos].append(scatter_send(2, pos, part, PARTS))

    for h in (0, 1):
        last2[h].wait_recv()

        def body(p_ref, l_ref, u0_ref, u1_ref, u2_ref, h=h):
            rows = pl.ds(pl.multiple_of(pl.program_id(0) * TILE, TILE), TILE)
            base[h, rows, :] = p_ref[...] + l_ref[...]
            usum[h, rows, :] = (u0_ref[...].astype(F32) + u1_ref[...].astype(F32)) + u2_ref[...].astype(F32)
        pltpu.emit_pipeline(body, grid=(half // TILE,), in_specs=[tile_spec] * 5)(
            pbuf.at[2, 6 + h], precv.at[2, 4 + h], user0.at[h], upan.at[1, 6 + h], upan.at[2, 6 + h])
    yrow.wait_recv()
    finish(core)
    selb[r] = sel[1] + selrecv[2]
    back = send(selb.at[r], selrecv.at[3], 'r', e_send.at[3], e_recv.at[3])
    back.wait_recv()

    user_base = ((r * 2 + y) * 2 + x) * (2 * half)
    local = idcol[0, :, 0:1] - user_base
    mine[...] = jnp.zeros_like(mine)
    size = half // PARTS
    for part in range(PARTS):
        rows = pl.ds(part * size, size)
        for h in (0, 1):
            parts[2 + h][part].wait_recv()
            last_user = (base[h, rows, :] + nearv[h, rows, :]).astype(BF16)
            mean = ((usum[h, rows, :] + last_user.astype(F32)) / (LAYERS + 1)).astype(BF16)
            user_out[h, rows, :] = mean
            hit = (local - (h * half + part * size)) == lax.broadcasted_iota(jnp.int32, (batch, size), 1)
            mine[...] += jnp.dot(hit.astype(BF16), mean, preferred_element_type=F32)
    own_rows, other_rows = selb[r].astype(F32), selrecv[3].astype(F32)
    pos_rows = jnp.where(r == 0, own_rows, other_rows)
    neg_rows = jnp.where(r == 0, other_rows, own_rows)
    rows = mine[...]
    margin = (jnp.sum(rows * pos_rows, axis=1, keepdims=True) - jnp.sum(rows * neg_rows, axis=1, keepdims=True)) / math.sqrt(dim)
    soft = jnp.maximum(-margin, 0.0) + jnp.log1p(jnp.exp(-jnp.abs(margin)))
    terms = jnp.where((local >= 0) & (local < 2 * half), soft, 0.0)
    lsend[...] = jnp.broadcast_to(jnp.sum(terms, axis=0, keepdims=True), (8, LANES))
    shared = [send_to(lsend, lrecv.at[i], device, l_send, l_recv.at[i], True) for i, device in enumerate(others)]
    for copy in pending:
        copy.wait_send()
    for k in range(LAYERS):
        wait_sent(upan.at[k, pl.ds(0, 6)], ag_send.at[k], ag_recv.at[k, 0])
        wait_sent(pbuf.at[k, pl.ds(0, 6)], rs_send.at[k], rs_recv.at[k, 0])
    wait_sent(lrecv, l_send, l_recv.at[0])
    wait_all(shared)
    level = [lsend[...]] + [lrecv[i] for i in range(len(others))]
    while len(level) > 1:
        level = [level[i] + level[i + 1] for i in range(0, len(level), 2)]
    loss_out[...] = level[0][0:1, 0:1] / batch


def solution(mesh):
    def device_program(mask_blk, user_shard, item_shard, triples):
        shard, dim = user_shard.shape
        half, items, own_items, batch = shard // 2, mask_blk.shape[1], item_shard.shape[0], triples.shape[0]
        hbm = pl.BlockSpec(memory_space=pltpu.HBM)
        vmem = pl.BlockSpec(memory_space=pltpu.VMEM)
        shapes = [((2, half, dim), BF16), ((own_items, dim), BF16), ((1, 1), F32), ((8, half, items), BF16),
                  ((LAYERS, 8, half, dim), BF16), ((LAYERS, 8, half, dim), F32), ((LAYERS, 6, half, dim), F32),
                  ((LAYERS, 2, half, dim), F32)]
        dma = pltpu.SemaphoreType.DMA
        outs = pl.pallas_call(
            functools.partial(kernel, (half, items, own_items, dim)),
            out_shape=[jax.ShapeDtypeStruct(*shape) for shape in shapes],
            in_specs=[hbm] * 4,
            out_specs=[vmem, vmem, vmem] + [hbm] * 5,
            scratch_shapes=[
                pltpu.VMEM((LAYERS, 2, own_items, dim), BF16), pltpu.VMEM((2, dim, own_items), F32),
                pltpu.VMEM((LAYERS, dim, own_items), F32), pltpu.VMEM((own_items, dim), F32),
                pltpu.VMEM((8, 8, BUILD), F32), pltpu.VMEM((BUILD, LANES), F32), pltpu.VMEM((1, items), F32),
                pltpu.VMEM((8, 8, BUILD), F32), pltpu.VMEM((2, 8, 8, BUILD), F32),
                pltpu.VMEM((8, items), F32), pltpu.VMEM((8, items), F32),
                pltpu.VMEM((2, batch, dim), BF16), pltpu.VMEM((2, batch, dim), BF16), pltpu.VMEM((4, batch, dim), BF16),
                pltpu.VMEM((batch, dim), F32), pltpu.VMEM((8, LANES), F32), pltpu.VMEM((7, 8, LANES), F32),
                pltpu.VMEM((3, batch), jnp.int32), pltpu.VMEM((3, batch, LANES), jnp.int32),
                pltpu.VMEM((2, half, dim), F32), pltpu.VMEM((2, half, dim), F32), pltpu.VMEM((2, half, dim), F32),
                dma((2,)),
                dma((LAYERS,)), dma((LAYERS, 6)), dma((LAYERS,)), dma((LAYERS, 6)), dma((2 * PARTS + 1,)), dma((LAYERS,)), dma((LAYERS,)),
                dma((LAYERS,)), dma((LAYERS,)), dma((4,)), dma((4,)), dma((4,)), dma((4,)), dma(()), dma((7,))],
            compiler_params=pltpu.CompilerParams(collective_id=0, has_side_effects=True, vmem_limit_bytes=48 * 1024 * 1024),
        )(*[pltpu.with_memory_space_constraint(a, pltpu.HBM) for a in (mask_blk, user_shard.reshape(2, half, dim), item_shard, triples.T)])
        return outs[0].reshape(shard, dim), outs[1], outs[2].reshape(())

    return jax.shard_map(device_program, mesh=mesh, in_specs=(P('row', COL_AXES), P(USER_AXES, None), P(ITEM_AXES, None), P()), out_specs=(P(USER_AXES, None), P(ITEM_AXES, None), P()), check_vma=False)
```

```python
import functools
import itertools
import math
import jax
import jax.numpy as jnp
from jax import lax
from jax.experimental import pallas as pl
from jax.experimental.pallas import tpu as pltpu
from jax.sharding import PartitionSpec as P

LAYERS = 3
USER_AXES = ('row', 'cola', 'colb')
ITEM_AXES = ('cola', 'colb', 'row')
COL_AXES = ('cola', 'colb')
F32 = jnp.float32
BF16 = jnp.bfloat16
CONTRACT_ROWS = (((0,), (0,)), ((), ()))
CONTRACT_COLS = (((1,), (1,)), ((), ()))
BUILD = 256
TILE = 512
CHUNK = 32
PARTS = 4
HEAD = 320
DEEP = pl.Buffered(4)
OUT = pl.Buffered(2)
LANES = 128


def kernel(dims, mask, user0, item0, triples, user_out, item_out, loss_out, adj, upan, pbuf, precv, sbuf,
           vpan, acc, qrecv, vtot, us, uscol, isc, degu, drecv, degi, degi_recv, sel, selb, selrecv, mine, lsend, lrecv,
           ids, idcol, base, usum, nearv, local_sem,
           ag_send, ag_recv, rs_send, rs_recv, p_recv, v_send, v_recv, q_send, q_recv, d_send, d_recv, e_send, e_recv, l_send, l_recv):
    half, items, own_items, dim = dims
    x, y, r = lax.axis_index('colb'), lax.axis_index('cola'), lax.axis_index('row')
    to = {'x': {'colb': 1 - x}, 'y': {'cola': 1 - y}, 'r': {'row': 1 - r},
          'xy': {'colb': 1 - x, 'cola': 1 - y}}
    others = [{'cola': 1 - y if dy else y, 'colb': 1 - x if dx else x, 'row': 1 - r if dr else r}
              for dy, dx, dr in itertools.product((0, 1), repeat=3) if dy or dx or dr]
    pending = []
    batch = ids.shape[1]

    def send_to(src, dst, device, send_sem, recv_sem, shared=False):
        copy = pltpu.make_async_remote_copy(src_ref=src, dst_ref=dst, send_sem=send_sem, recv_sem=recv_sem,
                                            device_id=device, device_id_type=pl.DeviceIdType.MESH)
        copy.start()
        if not shared:
            pending.append(copy)
        return copy

    def send(src, dst, direction, send_sem, recv_sem, shared=False):
        return send_to(src, dst, to[direction], send_sem, recv_sem, shared)

    def wait_sent(ref, send_sem, recv_sem):
        pltpu.make_async_remote_copy(src_ref=ref, dst_ref=ref, send_sem=send_sem, recv_sem=recv_sem,
                                     device_id=to['x'], device_id_type=pl.DeviceIdType.MESH).wait_send()

    def finish(copy):
        copy.wait_send()
        pending[:] = [other for other in pending if other is not copy]

    item_in = pltpu.make_async_copy(item0, vpan.at[0, r], local_sem.at[0])
    ids_in = pltpu.make_async_copy(triples, ids, local_sem.at[1])
    item_in.start()
    ids_in.start()
    barrier = pltpu.get_barrier_semaphore()
    for device in others:
        pl.semaphore_signal(barrier, inc=1, device_id=device, device_id_type=pl.DeviceIdType.MESH)
    pl.semaphore_wait(barrier, len(others))

    def own(k, h):
        return user0.at[h] if k == 0 else upan.at[k, 6 + h]

    def gather_start(k):
        return [send(own(k, 0), upan.at[k, 2], 'x', ag_send.at[k], ag_recv.at[k, 0], True),
                send(own(k, 1), upan.at[k, 3], 'y', ag_send.at[k], ag_recv.at[k, 1], True),
                send(own(k, 0), upan.at[k, 4], 'y', ag_send.at[k], ag_recv.at[k, 2], True),
                send(own(k, 1), upan.at[k, 5], 'x', ag_send.at[k], ag_recv.at[k, 3], True)]

    def gather_forward(k, copies):
        copies[0].wait_recv()
        far0 = send(upan.at[k, 2], upan.at[k, 0], 'y', ag_send.at[k], ag_recv.at[k, 4], True)
        copies[1].wait_recv()
        far1 = send(upan.at[k, 3], upan.at[k, 1], 'x', ag_send.at[k], ag_recv.at[k, 5], True)
        return copies[2:] + [far0, far1]

    def wait_all(copies):
        for copy in copies:
            copy.wait_recv()

    gather0 = gather_start(0)
    item_in.wait()
    ids_in.wait()
    item_copy = send(item0, vpan.at[0, r], 'r', v_send.at[0], v_recv.at[0])

    def mask_block(pos, tile):
        h, q = lax.rem(pos, 2), lax.div(pos, 2)
        prim, sec = 1 - lax.div(q, 2), 1 - lax.rem(q, 2)
        dx, dy = prim * (1 - h) + sec * h, sec * (1 - h) + prim * h
        shard = lax.rem(y + dy, 2) * 2 + lax.rem(x + dx, 2)
        return (shard * 2 + h) * (half // BUILD) + tile

    degu[...] = jnp.zeros_like(degu)
    degi[...] = jnp.zeros_like(degi)
    acc[...] = jnp.zeros_like(acc)

    def degree_body(m_ref):
        pos, tile = pl.program_id(0), pl.program_id(1)

        def chunk(i, cols):
            m = m_ref[pl.ds(pl.multiple_of(i * CHUNK, CHUNK), CHUNK), :]
            part = m[:, :LANES]
            for j in range(1, items // LANES):
                part = part + m[:, j * LANES:(j + 1) * LANES]
            uscol[pl.ds(pl.multiple_of(i * CHUNK, CHUNK), CHUNK), :] = part.astype(F32)
            for j in range(CHUNK // 8):
                cols = cols + m[j * 8:(j + 1) * 8, :]
            return cols

        cols = lax.fori_loop(0, BUILD // CHUNK, chunk, jnp.zeros((8, items), jnp.int32))
        degi[...] += cols.astype(F32)
        pick = (lax.broadcasted_iota(jnp.int32, (8, LANES), 0) == tile).astype(BF16)
        degu[pos] += lax.dot_general(pick, uscol[...].astype(BF16), CONTRACT_COLS, preferred_element_type=F32)

    pltpu.emit_pipeline(degree_body, grid=(8, half // BUILD),
                        in_specs=[pl.BlockSpec((BUILD, items), lambda p, t: (mask_block(p, t), 0), pipeline_mode=DEEP)])(mask)
    item_deg = send(degi, degi_recv, 'r', d_send.at[0], d_recv.at[0])
    user_deg = send(degu, drecv.at[0], 'x', d_send.at[1], d_recv.at[1])
    head, tail = pl.ds(0, HEAD), pl.ds(HEAD, half - HEAD)
    gather0[0].wait_recv()
    rest0 = gather0[2:] + [send(upan.at[0, 2, head], upan.at[0, 0, head], 'y', ag_send.at[0], ag_recv.at[0, 4], True)]
    gather0[1].wait_recv()
    rest0.append(send(upan.at[0, 3], upan.at[0, 1], 'x', ag_send.at[0], ag_recv.at[0, 5], True))
    user_deg.wait_recv()
    for pos in range(8):
        us[pos] = degu[pos] + drecv[0, pos ^ (2 if pos % 2 else 4)]
    user_deg2 = send(us, drecv.at[1], 'y', d_send.at[2], d_recv.at[2])
    rest0.append(send(upan.at[0, 2, tail], upan.at[0, 0, tail], 'y', ag_send.at[0], d_recv.at[3], True))
    item_deg.wait_recv()
    total = jnp.sum(degi[...] + degi_recv[...], axis=0, keepdims=True)
    isc[...] = lax.rsqrt(jnp.maximum(total, 1.0))
    user_deg2.wait_recv()
    finish(user_deg)
    for pos in range(8):
        degu[pos] = lax.rsqrt(jnp.maximum(us[pos] + drecv[1, pos ^ (4 if pos % 2 else 2)], 1.0))
    item_copy.wait_recv()

    def panel(k):
        return vpan[k].reshape(items, dim)

    def add_items(a_ref, u_ref):
        for j in range(2):
            acc[j] += lax.dot_general(u_ref[...], a_ref[:, j * own_items:(j + 1) * own_items], CONTRACT_ROWS,
                                      preferred_element_type=F32)

    def build(first, count, users, start_tile=0, tiles=half // BUILD):
        def body(m_ref, *refs):
            (u_ref, a_ref, p_ref) = refs if users is not None else (None,) + refs
            pos, tile = pl.program_id(0) + first, pl.program_id(1) + start_tile
            row = degu[pos, pl.ds(tile, 1), :]
            uscol[...] = jnp.transpose(jnp.broadcast_to(row, (LANES, BUILD)))

            def chunk(i, carry):
                rows = pl.ds(pl.multiple_of(i * CHUNK, CHUNK), CHUNK)
                scale = uscol[rows, :]
                for j in range(items // LANES):
                    cols = slice(j * LANES, (j + 1) * LANES)
                    weight = (scale * m_ref[rows, cols].astype(F32)) * isc[:, cols]
                    a_ref[rows, cols] = weight.astype(BF16)
                return carry

            lax.fori_loop(0, BUILD // CHUNK, chunk, 0)
            p_ref[...] = jnp.dot(a_ref[...], panel(0), preferred_element_type=F32)
            if users is not None:
                add_items(a_ref, u_ref)

        operands = [mask]
        in_specs = [pl.BlockSpec((BUILD, items), lambda p, t: (mask_block(p + first, t + start_tile), 0), pipeline_mode=DEEP)]
        if users is not None:
            ref, start = users
            operands.append(ref)
            in_specs.append(pl.BlockSpec((None, BUILD, dim), lambda p, t: (p + (first - start), t + start_tile, 0), pipeline_mode=DEEP))
        pltpu.emit_pipeline(body, grid=(count, tiles), in_specs=in_specs,
                            out_specs=[pl.BlockSpec((None, BUILD, items), lambda p, t: (p + first, t + start_tile, 0), pipeline_mode=OUT),
                                       pl.BlockSpec((None, BUILD, dim), lambda p, t: (p + first, t + start_tile, 0), pipeline_mode=OUT)])(*operands, adj, pbuf.at[0])

    def multiply(k, first, count):
        def body(a_ref, p_ref):
            p_ref[...] = jnp.dot(a_ref[...], panel(k), preferred_element_type=F32)
        pltpu.emit_pipeline(body, grid=(count, half // TILE),
                            in_specs=[pl.BlockSpec((None, TILE, items), lambda p, t: (p + first, t, 0), pipeline_mode=DEEP)],
                            out_specs=[pl.BlockSpec((None, TILE, dim), lambda p, t: (p + first, t, 0), pipeline_mode=OUT)])(adj, pbuf.at[k])

    def accumulate(k, count):
        pltpu.emit_pipeline(add_items, grid=(count, half // TILE),
                            in_specs=[pl.BlockSpec((None, TILE, items), lambda p, t: (p, t, 0), pipeline_mode=DEEP),
                                      pl.BlockSpec((None, TILE, dim), lambda p, t: (p, t, 0), pipeline_mode=DEEP)])(adj, upan.at[k])

    def scatter_send(k, pos, part=0, parts=1):
        rows = pl.ds(part * (half // parts), half // parts)
        last = k == LAYERS - 1 and pos >= 2
        dst = nearv.at[pos - 2, rows] if last else precv.at[k, pos, rows]
        index = (pos - 2) * PARTS + part if last else 2 * PARTS + part - 1
        recv_sem = rs_recv.at[k, pos] if part == 0 and not last else p_recv.at[index]
        return send(pbuf.at[k, pos, rows], dst, 'y' if pos % 2 else 'x', rs_send.at[k], recv_sem, True)

    tile_spec = pl.BlockSpec((TILE, dim), lambda t: (t, 0), pipeline_mode=DEEP)
    out_spec = pl.BlockSpec((TILE, dim), lambda t: (t, 0), pipeline_mode=OUT)

    def scatter_last(k, h, far):
        wait_all(far)

        def body(p_ref, r_ref, s_ref):
            s_ref[...] = p_ref[...] + r_ref[...]
        pltpu.emit_pipeline(body, grid=(half // TILE,), in_specs=[tile_spec] * 2, out_specs=[out_spec])(
            pbuf.at[k, 4 + h], precv.at[k, h], sbuf.at[k, h])
        return send(sbuf.at[k, h], precv.at[k, 4 + h], 'x' if h else 'y', rs_send.at[k], rs_recv.at[k, 4 + h], True)

    def scatter_finish(k, h, near, last):
        near.wait_recv()
        last.wait_recv()

        def body(p_ref, n_ref, l_ref, u_ref):
            u_ref[...] = ((p_ref[...] + n_ref[...]) + l_ref[...]).astype(BF16)
        pltpu.emit_pipeline(body, grid=(half // TILE,), in_specs=[tile_spec] * 3, out_specs=[out_spec])(
            pbuf.at[k, 6 + h], precv.at[k, 2 + h], precv.at[k, 4 + h], upan.at[k + 1, 6 + h])

    def item_layer(k):
        copy = send(acc.at[1 - r], qrecv.at[k - 1], 'r', q_send.at[k - 1], q_recv.at[k - 1])
        copy.wait_recv()
        rows = jnp.transpose(acc[r] + qrecv[k - 1]).astype(BF16)
        vtot[...] += rows.astype(F32)
        finish(copy)
        if k < LAYERS:
            vpan[k, r] = rows
            other = send(vpan.at[k, r], vpan.at[k, r], 'r', v_send.at[k], v_recv.at[k])
            acc[...] = jnp.zeros_like(acc)
            other.wait_recv()

    vtot[...] = vpan[0, r].astype(F32)
    for j in range(3):
        row = jnp.broadcast_to(ids[j:j + 1, :].astype(F32), (LANES, batch))
        idcol[j] = jnp.transpose(row).astype(jnp.int32)
    far, near = {}, {}
    build(0, 1, None)
    far[0, 0] = [scatter_send(0, 0)]
    far[0, 1] = []
    for part in range(2):
        build(1, 1, None, part * (half // BUILD // 2), half // BUILD // 2)
        far[0, 1].append(scatter_send(0, 1, part, 2))
    build(2, 1, (upan.at[0], 0))
    near[0, 0] = scatter_send(0, 2)
    build(3, 1, (upan.at[0], 0))
    near[0, 1] = scatter_send(0, 3)
    wait_all(rest0[:2])
    build(4, 2, (upan.at[0], 0))
    build(6, 2, (user0, 6))
    wait_all(rest0[2:])
    last0 = [scatter_last(0, h, far[0, h]) for h in (0, 1)]
    accumulate(0, 2)
    item_layer(1)
    for pos in range(2):
        multiply(1, pos, 1)
        far[1, pos] = [scatter_send(1, pos)]
    multiply(1, 2, 6)
    for h in (0, 1):
        scatter_finish(0, h, near[0, h], last0[h])
    gather1 = gather_start(1)
    rest1 = gather_forward(1, gather1)
    for pos in (2, 3):
        near[1, pos % 2] = scatter_send(1, pos)
    last1 = [scatter_last(1, h, far[1, h]) for h in (0, 1)]
    wait_all(rest1)
    accumulate(1, 8)
    item_layer(2)
    for pos in range(2):
        multiply(2, pos, 1)
        far[2, pos] = [scatter_send(2, pos)]
    multiply(2, 2, 6)
    for h in (0, 1):
        scatter_finish(1, h, near[1, h], last1[h])
    gather2 = gather_start(2)
    rest2 = gather_forward(2, gather2)
    last2 = [scatter_last(2, h, far[2, h]) for h in (0, 1)]
    wait_all(rest2)
    accumulate(2, 8)
    item_layer(3)

    out_rows = (vtot[...] / (LAYERS + 1)).astype(BF16)
    item_out[...] = out_rows
    item_base = ((y * 2 + x) * 2 + r) * own_items
    for j in range(2):
        hit = (idcol[1 + j, :, 0:1] - item_base) == lax.broadcasted_iota(jnp.int32, (batch, own_items), 1)
        selb[j] = jnp.dot(hit.astype(BF16), out_rows, preferred_element_type=F32).astype(BF16)
    core = send(selb.at[1 - r], selrecv.at[0], 'r', e_send.at[0], e_recv.at[0])
    core.wait_recv()
    sel[0] = selb[r] + selrecv[0]
    xrow = send(sel.at[0], selrecv.at[1], 'x', e_send.at[1], e_recv.at[1])
    parts = {2: [scatter_send(2, 2, 0, PARTS)], 3: [scatter_send(2, 3, 0, PARTS)]}
    xrow.wait_recv()
    sel[1] = sel[0] + selrecv[1]
    yrow = send(sel.at[1], selrecv.at[2], 'y', e_send.at[2], e_recv.at[2])
    for part in range(1, PARTS):
        for pos in (2, 3):
            parts[pos].append(scatter_send(2, pos, part, PARTS))

    for h in (0, 1):
        last2[h].wait_recv()

        def body(p_ref, l_ref, u0_ref, u1_ref, u2_ref, h=h):
            rows = pl.ds(pl.multiple_of(pl.program_id(0) * TILE, TILE), TILE)
            base[h, rows, :] = p_ref[...] + l_ref[...]
            usum[h, rows, :] = (u0_ref[...].astype(F32) + u1_ref[...].astype(F32)) + u2_ref[...].astype(F32)
        pltpu.emit_pipeline(body, grid=(half // TILE,), in_specs=[tile_spec] * 5)(
            pbuf.at[2, 6 + h], precv.at[2, 4 + h], user0.at[h], upan.at[1, 6 + h], upan.at[2, 6 + h])
    yrow.wait_recv()
    finish(core)
    selb[r] = sel[1] + selrecv[2]
    back = send(selb.at[r], selrecv.at[3], 'r', e_send.at[3], e_recv.at[3])
    back.wait_recv()

    user_base = ((r * 2 + y) * 2 + x) * (2 * half)
    local = idcol[0, :, 0:1] - user_base
    mine[...] = jnp.zeros_like(mine)
    size = half // PARTS
    for part in range(PARTS):
        rows = pl.ds(part * size, size)
        for h in (0, 1):
            parts[2 + h][part].wait_recv()
            last_user = (base[h, rows, :] + nearv[h, rows, :]).astype(BF16)
            mean = ((usum[h, rows, :] + last_user.astype(F32)) / (LAYERS + 1)).astype(BF16)
            user_out[h, rows, :] = mean
            hit = (local - (h * half + part * size)) == lax.broadcasted_iota(jnp.int32, (batch, size), 1)
            mine[...] += jnp.dot(hit.astype(BF16), mean, preferred_element_type=F32)
    own_rows, other_rows = selb[r].astype(F32), selrecv[3].astype(F32)
    pos_rows = jnp.where(r == 0, own_rows, other_rows)
    neg_rows = jnp.where(r == 0, other_rows, own_rows)
    rows = mine[...]
    margin = (jnp.sum(rows * pos_rows, axis=1, keepdims=True) - jnp.sum(rows * neg_rows, axis=1, keepdims=True)) / math.sqrt(dim)
    soft = jnp.maximum(-margin, 0.0) + jnp.log1p(jnp.exp(-jnp.abs(margin)))
    terms = jnp.where((local >= 0) & (local < 2 * half), soft, 0.0)
    lsend[...] = jnp.broadcast_to(jnp.sum(terms, axis=0, keepdims=True), (1, LANES))
    shared = [send_to(lsend, lrecv.at[i], device, l_send, l_recv.at[i], True) for i, device in enumerate(others)]
    for copy in pending:
        copy.wait_send()
    for k in range(LAYERS):
        wait_sent(upan.at[k, pl.ds(0, 6)], ag_send.at[k], ag_recv.at[k, 0])
        wait_sent(pbuf.at[k, pl.ds(0, 6)], rs_send.at[k], rs_recv.at[k, 0])
    wait_sent(lrecv, l_send, l_recv.at[0])
    wait_all(shared)
    level = [lsend[...]] + [lrecv[i] for i in range(len(others))]
    while len(level) > 1:
        level = [level[i] + level[i + 1] for i in range(0, len(level), 2)]
    loss_out[...] = level[0][0:1, 0:1] / batch


def solution(mesh):
    def device_program(mask_blk, user_shard, item_shard, triples):
        shard, dim = user_shard.shape
        half, items, own_items, batch = shard // 2, mask_blk.shape[1], item_shard.shape[0], triples.shape[0]
        hbm = pl.BlockSpec(memory_space=pltpu.HBM)
        vmem = pl.BlockSpec(memory_space=pltpu.VMEM)
        shapes = [((2, half, dim), BF16), ((own_items, dim), BF16), ((1, 1), F32), ((8, half, items), BF16),
                  ((LAYERS, 8, half, dim), BF16), ((LAYERS, 8, half, dim), F32), ((LAYERS, 6, half, dim), F32),
                  ((LAYERS, 2, half, dim), F32)]
        dma = pltpu.SemaphoreType.DMA
        outs = pl.pallas_call(
            functools.partial(kernel, (half, items, own_items, dim)),
            out_shape=[jax.ShapeDtypeStruct(*shape) for shape in shapes],
            in_specs=[hbm] * 4,
            out_specs=[vmem, vmem, vmem] + [hbm] * 5,
            scratch_shapes=[
                pltpu.VMEM((LAYERS, 2, own_items, dim), BF16), pltpu.VMEM((2, dim, own_items), F32),
                pltpu.VMEM((LAYERS, dim, own_items), F32), pltpu.VMEM((own_items, dim), F32),
                pltpu.VMEM((8, 8, BUILD), F32), pltpu.VMEM((BUILD, LANES), F32), pltpu.VMEM((1, items), F32),
                pltpu.VMEM((8, 8, BUILD), F32), pltpu.VMEM((2, 8, 8, BUILD), F32),
                pltpu.VMEM((8, items), F32), pltpu.VMEM((8, items), F32),
                pltpu.VMEM((2, batch, dim), BF16), pltpu.VMEM((2, batch, dim), BF16), pltpu.VMEM((4, batch, dim), BF16),
                pltpu.VMEM((batch, dim), F32), pltpu.VMEM((1, LANES), F32), pltpu.VMEM((7, 1, LANES), F32),
                pltpu.VMEM((3, batch), jnp.int32), pltpu.VMEM((3, batch, LANES), jnp.int32),
                pltpu.VMEM((2, half, dim), F32), pltpu.VMEM((2, half, dim), F32), pltpu.VMEM((2, half, dim), F32),
                dma((2,)),
                dma((LAYERS,)), dma((LAYERS, 6)), dma((LAYERS,)), dma((LAYERS, 6)), dma((2 * PARTS + 1,)), dma((LAYERS,)), dma((LAYERS,)),
                dma((LAYERS,)), dma((LAYERS,)), dma((4,)), dma((4,)), dma((4,)), dma((4,)), dma(()), dma((7,))],
            compiler_params=pltpu.CompilerParams(collective_id=0, has_side_effects=True, vmem_limit_bytes=48 * 1024 * 1024),
        )(*[pltpu.with_memory_space_constraint(a, pltpu.HBM) for a in (mask_blk, user_shard.reshape(2, half, dim), item_shard, triples.T)])
        return outs[0].reshape(shard, dim), outs[1], outs[2].reshape(())

    return jax.shard_map(device_program, mesh=mesh, in_specs=(P('row', COL_AXES), P(USER_AXES, None), P(ITEM_AXES, None), P()), out_specs=(P(USER_AXES, None), P(ITEM_AXES, None), P()), check_vma=False)
```
